32 devices in a mesh: site: 2 (over y), rows: 8 (over z, core), width: 2 (over x).
Axes of the slice: x: 2, y: 2, z: 4, core: 2. Of those that a mesh axis runs over, the one named last changes fastest.
Arguments:
- one_query: float32 [14336, 7168], P(('site', 'rows'), 'width'), parts along dimension 0, may hold values from -0.09375 to 0.09375
- other_query: float32 [14336, 7168], P(('site', 'rows'), 'width'), parts along dimension 0, may hold values from -0.0625 to 0.0625
- one_key: float32 [14336, 1024], P(('site', 'rows'), 'width'), parts along dimension 0, may hold values from -0.09375 to 0.09375
- other_key: float32 [14336, 1024], P(('site', 'rows'), 'width'), parts along dimension 0, may hold values from -0.0625 to 0.0625
- one_value: float32 [14336, 1024], P(('site', 'rows'), 'width'), parts along dimension 0, may hold values from -0.09375 to 0.09375
- other_value: float32 [14336, 1024], P(('site', 'rows'), 'width'), parts along dimension 0, may hold values from -0.0625 to 0.0625
- mix_share: float32 [14336], P(('site', 'rows')), parts along dimension 0, may hold values from 0.2 to 0.8
- norm_train: float32 [14336], P(('site', 'rows', 'width')), parts along dimension 0, may hold values from 0.25 to 1.75
- norm_step: float32 [14336], P(('site', 'rows', 'width')), parts along dimension 0, may hold values from -0.3 to 0.3
Outputs:
- serving_query: bfloat16 [14336, 7168], P('site', 'width'), parts along dimension 0
- serving_key: bfloat16 [14336, 1024], P('site', 'width'), parts along dimension 0
- serving_value: bfloat16 [14336, 1024], P('site', 'width'), parts along dimension 0
- scale_query: float32 [14336], P(('site', 'width')), parts along dimension 0
- scale_key: float32 [2048], P(('site', 'width')), parts along dimension 0
- scale_value: float32 [2048], P(('site', 'width')), parts along dimension 0
- serve_norm: bfloat16 [14336], P('site'), parts along dimension 0
The draws below stay inside these ranges and needn't reach their ends.
There are 2 independent parts, one for each index of `site`. The reference program is written for one: setup_inputs(seed, part) draws one part's arguments, and reference() takes and returns one part's arrays. A program takes and returns all parts, laid end to end along the dimension named above; each array names one. Nothing has to cross between parts.
All inputs are finite; a program needn't handle non-finite values. Where the reference program divides by a largest or mean magnitude, that divisor is 1e-20 or more.
Results may differ from the reference program's by a relative error of at most 0.001.
Values may be sent and summed in bfloat16 or wider, within the bound.
A program may use at most 256 MiB of HBM per device.

```python
import jax
import jax.numpy as jnp

D_MODEL = 7168
Q_DIM = 7168
KV_DIM = 1024


def raised(drawn, rng, source, target, blocks, factor):
    def block_of(dim):
        return (jnp.arange(drawn.shape[dim]) // (drawn.shape[dim] // blocks)).reshape((-1,) + (1,) * (drawn.ndim - 1 - dim))

    first = jax.random.permutation(rng, blocks)[block_of(target)]
    other_side = (block_of(target) + blocks // 2) % blocks
    return jnp.where((block_of(source) == first) | (block_of(source) == other_side), factor * drawn, drawn)


def level_of(own_key, dims, cuts, least, largest):
    loudness = 1.0
    for position, blocks in cuts:
        heights = jax.random.uniform(jax.random.fold_in(jax.random.fold_in(own_key, 6), position), (blocks,), jnp.float32, least / len(cuts), largest / len(cuts))
        loudness = loudness * jnp.repeat(jnp.exp(heights), dims[position] // blocks).reshape((-1,) + (1,) * (len(dims) - 1 - position))
    return loudness


def gaussian(stream_key, shape, width, most, shards=(), kind=jnp.bfloat16):
    result = jax.random.normal(stream_key, shape, jnp.float32) * width
    if len(shards) > 0:
        result = level_of(stream_key, shape, shards, -0.22, 0.18) * result
    return jnp.clip(result, min=-most, max=most).astype(kind)


def bell_draw_with(stream_key, extent, spread, reach, cuts, heavy, dtype=jnp.bfloat16):
    result = spread * jax.random.normal(stream_key, extent, jnp.float32)
    if cuts:
        result = result * level_of(stream_key, extent, cuts, -0.22, 0.18)
    return jnp.clip(raised(result, jax.random.fold_in(stream_key, 3), *heavy), -reach, reach).astype(dtype)


def setup_inputs(seed: int = 0, part: int = 0) -> dict:
    seeds = jax.random.split(jax.random.key(seed), 10)
    part_splits = jax.random.split(jax.random.fold_in(seeds[9], part), 10)
    return {
        "one_query": bell_draw_with(part_splits[0], (D_MODEL, Q_DIM), D_MODEL ** -0.5, 0.09375, ((0, 8), (1, 2)), (0, 1, 8, 2.0), jnp.float32),
        "other_query": gaussian(part_splits[1], (D_MODEL, Q_DIM), D_MODEL ** -0.5, 0.0625, ((0, 8), (1, 2)), jnp.float32),
        "one_key": bell_draw_with(part_splits[2], (D_MODEL, KV_DIM), D_MODEL ** -0.5, 0.09375, ((0, 8), (1, 2)), (0, 1, 8, 2.0), jnp.float32),
        "other_key": gaussian(part_splits[3], (D_MODEL, KV_DIM), D_MODEL ** -0.5, 0.0625, ((0, 8), (1, 2)), jnp.float32),
        "one_value": bell_draw_with(part_splits[4], (D_MODEL, KV_DIM), D_MODEL ** -0.5, 0.09375, ((0, 8), (1, 2)), (0, 1, 8, 2.0), jnp.float32),
        "other_value": gaussian(part_splits[5], (D_MODEL, KV_DIM), D_MODEL ** -0.5, 0.0625, ((0, 8), (1, 2)), jnp.float32),
        "mix_share": jnp.clip(0.2 + 0.6 * jax.random.uniform(part_splits[6], (D_MODEL,), jnp.float32) ** level_of(part_splits[6], (D_MODEL,), ((0, 8),), -0.2, 0.2), 0.2, 0.8),
        "norm_train": jnp.clip(1.0 + 0.15 * jax.random.normal(part_splits[7], (D_MODEL,), jnp.float32), 0.25, 1.75),
        "norm_step": jnp.clip(jax.random.uniform(part_splits[8], (D_MODEL,), jnp.float32, -0.3, 0.3) * level_of(part_splits[8], (D_MODEL,), ((0, 16),), -0.4, 0.0), -0.3, 0.3),
    }


def reference(one_query, other_query, one_key, other_key, one_value, other_value, mix_share, norm_train, norm_step):
    whole_query = mix_share[:, None] * one_query + (1.0 - mix_share[:, None]) * other_query
    whole_key = mix_share[:, None] * one_key + (1.0 - mix_share[:, None]) * other_key
    whole_value = mix_share[:, None] * one_value + (1.0 - mix_share[:, None]) * other_value
    scale_query = jnp.max(jnp.abs(whole_query), axis=0)
    serving_query = (whole_query / scale_query).astype(jnp.bfloat16)
    scale_key = jnp.max(jnp.abs(whole_key), axis=0)
    serving_key = (whole_key / scale_key).astype(jnp.bfloat16)
    scale_value = jnp.max(jnp.abs(whole_value), axis=0)
    serving_value = (whole_value / scale_value).astype(jnp.bfloat16)
    serve_norm = (norm_train + norm_step).astype(jnp.bfloat16)
    return serving_query, serving_key, serving_value, scale_query, scale_key, scale_value, serve_norm
```

```python
import functools

import jax
import jax.numpy as jnp
from jax import lax
from jax.experimental import pallas as pl
from jax.experimental.pallas import tpu as pltpu
from jax.sharding import PartitionSpec as P


MESH = pl.DeviceIdType.MESH
CORES = 2
LANES = 128
LATE = 2
AHEAD = 3


def merge(
    ranks,
    widths,
    one_query,
    other_query,
    one_key,
    other_key,
    one_value,
    other_value,
    mix_row,
    norm_train,
    norm_step,
    query,
    key,
    value,
    far_query,
    far_key,
    far_value,
    scale_query,
    scale_key,
    scale_value,
    norms,
    one,
    other,
    narrow,
    mix,
    peaks,
    load_sem,
    out_sem,
    far_sem,
    peak_send,
    peak_recv,
    norm_send,
    norm_recv,
    up_send,
    up_recv,
    down_send,
    down_recv,
    side_send,
    side_recv,
):
    depth, span = one_key.shape
    parts = one_query.shape[1] // span
    early = parts - LATE
    chips = ranks // CORES
    me = lax.axis_index("rows")
    across = lax.axis_index("width")
    chip, core = me // CORES, me % CORES
    partner = chip * CORES + 1 - core
    group = ranks * widths
    block = 32 if depth % 32 == 0 else depth
    late_parts = range(early, parts + 2)

    def is_static(k):
        return isinstance(k, int)

    def loads(k):
        if is_static(k) and k >= parts:
            sources = (one_key, other_key) if k == parts else (one_value, other_value)
        else:
            cut = pl.ds(pl.multiple_of(k * span, span), span)
            sources = one_query.at[:, cut], other_query.at[:, cut]
        return [
            pltpu.make_async_copy(source, target.at[k], load_sem.at[i, k])
            for i, (source, target) in enumerate(zip(sources, (one, other)))
        ]

    def load(k):
        for copy in loads(k):
            copy.start()

    pl.loop(0, AHEAD)(load)

    barrier = pltpu.get_barrier_semaphore()
    mine = me * widths + across

    @pl.loop(1, group)
    def _(step):
        to = lax.rem(mine + step, group)
        pl.semaphore_signal(
            barrier,
            inc=1,
            device_id={"rows": to // widths, "width": lax.rem(to, widths)},
            device_id_type=MESH,
        )

    norms[mine] = norm_train[...] + norm_step[...]

    for first in range(0, mix.shape[0], LANES):
        row = mix_row[:, first : first + LANES]
        mix[first : first + LANES] = jnp.broadcast_to(row, (LANES, LANES)).T

    def send_peaks(k):
        @pl.loop(1, ranks)
        def _(step):
            pltpu.make_async_remote_copy(
                src_ref=peaks.at[k, me],
                dst_ref=peaks.at[k, me],
                send_sem=peak_send.at[k],
                recv_sem=peak_recv.at[k],
                device_id={"rows": lax.rem(me + step, ranks)},
                device_id_type=MESH,
            ).start()

    def mixed(k):
        for copy in loads(k):
            copy.wait()
        if is_static(k):
            if k + AHEAD < parts + 2:
                load(k + AHEAD)
        else:

            @pl.when(k + AHEAD < parts)
            def _():
                load(k + AHEAD)

            for tail in (parts, parts + 1):

                @pl.when(k + AHEAD == tail)
                def _():
                    load(tail)

        def step(b, top):
            rows = pl.ds(pl.multiple_of(b * block, block), block)
            share = jnp.concatenate([mix[rows]] * (span // LANES), axis=1)
            whole = share * one[k, rows] + (1.0 - share) * other[k, rows]
            one[k, rows] = whole
            return jnp.maximum(top, jnp.max(jnp.abs(whole).reshape(-1, 8, span), axis=0))

        top = lax.fori_loop(0, depth // block, step, jnp.zeros((8, span), jnp.float32))
        peaks[k, me] = jnp.max(top, axis=0, keepdims=True)

    def is_tail(k):
        return is_static(k) and k >= parts

    def hops(k):
        return chips - 2 if is_static(k) and k >= early else chips - 1

    def slot(k, rank):
        rows = pl.ds(pl.multiple_of(rank * depth, depth), depth)
        if is_tail(k):
            return (key if k == parts else value).at[rows]
        return query.at[rows, pl.ds(pl.multiple_of(k * span, span), span)]

    def send(k, rank, to, send_sem, recv_sem, source=None):
        return pltpu.make_async_remote_copy(
            src_ref=slot(k, rank) if source is None else source,
            dst_ref=slot(k, rank),
            send_sem=send_sem,
            recv_sem=recv_sem,
            device_id={"rows": to},
            device_id_type=MESH,
        )

    def go_up(k, hop, source=None):
        return send(k, me - CORES * hop, me + CORES, up_send.at[hop, k], up_recv.at[hop, k], source)

    def go_down(k, hop, source=None):
        return send(
            k, me + CORES * hop, me - CORES, down_send.at[hop, k], down_recv.at[hop, k], source
        )

    def go_side(k, hop, source=None):
        index = hop + chips - 1
        return send(
            k, me + CORES * hop, partner, side_send.at[index, k], side_recv.at[index, k], source
        )

    def from_side(k, hop):
        index = hop + chips - 1
        return send(
            k, partner + CORES * hop, partner, side_send.at[index, k], side_recv.at[index, k]
        )

    def from_below(k, hop):
        return send(k, me - CORES * (hop + 1), me - CORES, up_send.at[hop, k], up_recv.at[hop, k])

    def from_above(k, hop):
        return send(
            k, me + CORES * (hop + 1), me + CORES, down_send.at[hop, k], down_recv.at[hop, k]
        )

    has_below, has_above = chip >= 1, chip < chips - 1

    def keep(k):
        return pltpu.make_async_copy(narrow.at[k], slot(k, me), out_sem.at[k])

    def scaled(k, scale_ref, cut):
        everyone = peaks.at[k, pl.ds(0, ranks - 1)]
        pltpu.make_async_copy(everyone, everyone, peak_recv.at[k]).wait()
        scale = jnp.max(peaks[k], axis=0)
        scale_ref[:, cut] = scale

        @pl.loop(0, depth // block)
        def _(b):
            rows = pl.ds(pl.multiple_of(b * block, block), block)
            narrow[k, rows] = (one[k, rows] / scale).astype(jnp.bfloat16)

        source = narrow.at[k]

        @pl.when(has_below)
        def _():
            go_down(k, 0, source).start()

        @pl.when(has_above)
        def _():
            go_up(k, 0, source).start()

        go_side(k, 0, source).start()
        keep(k).start()

    def part_cut(k):
        return pl.ds(pl.multiple_of(k * span, span), span)

    mixed(0)
    pl.semaphore_wait(barrier, group - 1)
    send_peaks(0)

    def advance(k):
        mixed(k)
        send_peaks(k)

    lag = min(2, parts)
    pl.loop(1, lag)(advance)

    @pl.loop(0, parts - lag)
    def _(k):
        advance(k + lag)
        scaled(k, scale_query, part_cut(k))

    advance(parts)
    advance(parts + 1)

    @pl.loop(1, group)
    def _(step):
        to = lax.rem(mine + step, group)
        pltpu.make_async_remote_copy(
            src_ref=norms.at[mine],
            dst_ref=norms.at[mine],
            send_sem=norm_send,
            recv_sem=norm_recv,
            device_id={"rows": to // widths, "width": lax.rem(to, widths)},
            device_id_type=MESH,
        ).start()

    @pl.loop(parts - lag, parts)
    def _(k):
        scaled(k, scale_query, part_cut(k))

    scaled(parts, scale_key, slice(None))
    scaled(parts + 1, scale_value, slice(None))

    def far_copy(k, rank):
        if is_tail(k):
            target = far_key if k == parts else far_value
        else:
            target = far_query.at[:, pl.ds((k - early) * span, span)]
        return pltpu.make_async_copy(slot(k, rank), target, far_sem.at[k - early])

    def relay(k, hop):
        onward = hop < hops(k)
        is_far = is_static(k) and k >= early

        @pl.when(chip >= hop)
        def _():
            from_below(k, hop - 1).wait_recv()

            @pl.when(has_above & onward)
            def _():
                go_up(k, hop).start()

            go_side(k, -hop).start()

            if is_far:

                @pl.when((hop == chips - 2) & (chip == chips - 2))
                def _():
                    far_copy(k, me - CORES * hop).start()

        @pl.when(chip + hop < chips)
        def _():
            from_above(k, hop - 1).wait_recv()

            @pl.when(has_below & onward)
            def _():
                go_down(k, hop).start()

            go_side(k, hop).start()

            if is_far:

                @pl.when((hop == chips - 2) & (chip == 1))
                def _():
                    far_copy(k, me + CORES * hop).start()

    @pl.loop(1, chips - 1)
    def _(hop):
        pl.loop(0, early)(lambda k: relay(k, hop))
        for k in late_parts:
            relay(k, hop)

    pl.loop(0, early)(lambda k: relay(k, chips - 1))

    def finish(k):
        keep(k).wait()

        @pl.loop(0, hops(k))
        def _(hop):
            @pl.when((chip >= hop) & has_above)
            def _():
                go_up(k, hop).wait_send()

            @pl.when((chip + hop < chips) & has_below)
            def _():
                go_down(k, hop).wait_send()

        @pl.loop(0, chips)
        def _(origin):
            @pl.when((origin - chip <= hops(k)) & (chip - origin <= hops(k)))
            def _():
                go_side(k, origin - chip).wait_send()
                from_side(k, origin - chip).wait_recv()

        if is_static(k):

            @pl.when((chip == 1) | (chip == chips - 2))
            def _():
                far_copy(k, me).wait()

    for k in late_parts:
        finish(k)

    def settle(k):
        everyone = peaks.at[k, pl.ds(0, ranks - 1)]
        pltpu.make_async_copy(everyone, everyone, peak_send.at[k]).wait()

    pl.loop(0, parts + 2)(settle)
    others = norms.at[pl.ds(0, group - 1)]
    pltpu.make_async_copy(others, others, norm_recv).wait()
    pltpu.make_async_copy(others, others, norm_send).wait()
    pl.loop(0, early)(finish)


def stream(total, incoming, outgoing, ring):
    ahead = ring // 2

    def head():
        for i in range(min(ahead, total)):
            incoming(i, True)

    def body():
        @pl.loop(0, total)
        def _(i):
            incoming(i, False)
            outgoing(i).start()

            @pl.when(i + ahead < total)
            def _():
                @pl.when(i + ahead >= ring)
                def _():
                    outgoing(i + ahead - ring).wait()

                incoming(i + ahead, True)

    def drain():
        @pl.loop(max(0, total - ring), total)
        def _(i):
            outgoing(i).wait()

    return head, body, drain


def act(copy, begin):
    if begin:
        copy.start()
    else:
        copy.wait()


def settle_kernel(query, value, new_query, new_value, done, wide_buf, slim_buf, sems):
    ring = wide_buf.shape[0]

    def plan(source, target, buf, at):
        step = buf.shape[1]
        cols = pl.ds(0, buf.shape[2])

        def rows(i):
            return pl.ds(pl.multiple_of(i * step, step), step)

        def incoming(i, begin):
            place = lax.rem(i, ring)
            act(
                pltpu.make_async_copy(
                    source.at[rows(i), cols], buf.at[place], sems.at[at, place]
                ),
                begin,
            )

        def outgoing(i):
            place = lax.rem(i, ring)
            return pltpu.make_async_copy(
                buf.at[place], target.at[rows(i), cols], sems.at[at + 1, place]
            )

        return stream(source.shape[0] // step, incoming, outgoing, ring)

    first = plan(query, new_query, wide_buf, 0)
    second = plan(value, new_value, slim_buf, 2)
    first[0]()
    first[1]()
    second[0]()
    second[1]()
    first[2]()
    second[2]()
    done[...] = jnp.zeros_like(done)


def chunk_of(rows, most):
    step = rows
    while step > most and step % 32 == 0:
        step //= 2
    return step


def settled(query, value, wide, ring=8):
    rows, span = value.shape
    step = chunk_of(rows, 128)
    slim = chunk_of(rows, 512)
    anywhere = pl.BlockSpec(memory_space=pl.ANY)
    moved = 4 * rows * (wide + span)
    return pl.pallas_call(
        settle_kernel,
        out_shape=(
            jax.ShapeDtypeStruct(query.shape, query.dtype),
            jax.ShapeDtypeStruct(value.shape, value.dtype),
            jax.ShapeDtypeStruct((8, LANES), jnp.float32),
        ),
        in_specs=[anywhere] * 2,
        out_specs=(anywhere, anywhere, pl.BlockSpec(memory_space=pltpu.VMEM)),
        scratch_shapes=[
            pltpu.VMEM((ring, step, wide), query.dtype),
            pltpu.VMEM((ring, slim, span), value.dtype),
            pltpu.SemaphoreType.DMA((4, ring)),
        ],
        compiler_params=pltpu.CompilerParams(vmem_limit_bytes=60 * 2**20),
        cost_estimate=pl.CostEstimate(
            flops=0, bytes_accessed=moved, transcendentals=0
        ),
    )(query, value)


def far_ranks(ranks):
    chips = ranks // CORES
    me = lax.axis_index("rows")
    chip, core = me // CORES, me % CORES
    at_end = (chip == 0) | (chip == chips - 1)
    away = jnp.where(chip == 0, chips - 1, 0) * CORES
    return at_end, away + core, away + 1 - core


def blend_kernel(
    ranks, wide, _, query, key, got_query, side_query, got_key, side_key, done,
    new_query, new_key, query_buf, key_buf, sems,
):
    depth = got_key.shape[0]
    at_end, straight, crossed = far_ranks(ranks)
    ring = query_buf.shape[0]
    late = query_buf.shape[2]

    def plan(source, got, side, target, buf, cols, at):
        def rows(i):
            return pl.ds(pl.multiple_of(i * depth, depth), depth)

        def incoming(i, begin):
            place = lax.rem(i, ring)

            def copy(origin):
                act(pltpu.make_async_copy(origin, buf.at[place], sems.at[at, place]), begin)

            if not begin:
                copy(source.at[rows(i), cols])
                return
            is_got = at_end & (i == straight)
            is_side = at_end & (i == crossed)
            pl.when(is_got)(lambda: copy(got))
            pl.when(is_side)(lambda: copy(side))
            pl.when(jnp.logical_not(is_got | is_side))(lambda: copy(source.at[rows(i), cols]))

        def outgoing(i):
            place = lax.rem(i, ring)
            return pltpu.make_async_copy(
                buf.at[place], target.at[rows(i), cols], sems.at[at + 1, place]
            )

        return stream(ranks, incoming, outgoing, ring)

    first = plan(
        query, got_query, side_query, new_query, query_buf, pl.ds(wide, late), 0
    )
    second = plan(key, got_key, side_key, new_key, key_buf, pl.ds(0, key_buf.shape[2]), 2)
    first[0]()
    second[0]()
    first[1]()
    second[1]()
    first[2]()
    second[2]()


def blended(
    ranks, wide, new_query, query, key, got_query, side_query, got_key, side_key, done, ring=4
):
    depth, span = got_key.shape
    late = got_query.shape[1]
    anywhere = pl.BlockSpec(memory_space=pl.ANY)
    moved = 4 * ranks * depth * (late + span)
    return pl.pallas_call(
        functools.partial(blend_kernel, ranks, wide),
        out_shape=(
            jax.ShapeDtypeStruct(query.shape, query.dtype),
            jax.ShapeDtypeStruct(key.shape, key.dtype),
        ),
        in_specs=[anywhere] * 8,
        out_specs=(anywhere, anywhere),
        scratch_shapes=[
            pltpu.VMEM((ring, depth, late), query.dtype),
            pltpu.VMEM((ring, depth, span), key.dtype),
            pltpu.SemaphoreType.DMA((4, ring)),
        ],
        input_output_aliases={0: 0},
        compiler_params=pltpu.CompilerParams(vmem_limit_bytes=60 * 2**20),
        cost_estimate=pl.CostEstimate(
            flops=0, bytes_accessed=moved, transcendentals=0
        ),
    )(new_query, query, key, got_query, side_query, got_key, side_key, done)


def place_kernel(ranks, _, got, side, target, buf, sems):
    at_end, straight, crossed = far_ranks(ranks)
    depth = got.shape[0]
    step = buf.shape[1]
    cuts = depth // step

    @pl.when(at_end)
    def _():
        def incoming(i):
            source = (got, side)[i // cuts]
            rows = pl.ds(i % cuts * step, step)
            return pltpu.make_async_copy(source.at[rows], buf.at[i], sems.at[0, i])

        def outgoing(i):
            rank = (straight, crossed)[i // cuts]
            rows = pl.ds(pl.multiple_of(rank * depth + i % cuts * step, step), step)
            return pltpu.make_async_copy(buf.at[i], target.at[rows], sems.at[1, i])

        for i in range(2 * cuts):
            incoming(i).start()
        for i in range(2 * cuts):
            incoming(i).wait()
            outgoing(i).start()
        for i in range(2 * cuts):
            outgoing(i).wait()


def placed(ranks, whole, got, side, cuts=4):
    depth, span = got.shape
    anywhere = pl.BlockSpec(memory_space=pl.ANY)
    return pl.pallas_call(
        functools.partial(place_kernel, ranks),
        out_shape=jax.ShapeDtypeStruct(whole.shape, whole.dtype),
        in_specs=[anywhere] * 3,
        out_specs=anywhere,
        scratch_shapes=[
            pltpu.VMEM((2 * cuts, depth // cuts, span), whole.dtype),
            pltpu.SemaphoreType.DMA((2, 2 * cuts)),
        ],
        input_output_aliases={0: 0},
        compiler_params=pltpu.CompilerParams(vmem_limit_bytes=8 * 2**20),
        cost_estimate=pl.CostEstimate(
            flops=0, bytes_accessed=8 * depth * span, transcendentals=0
        ),
    )(whole, got, side)


def shards(
    ranks,
    widths,
    one_query,
    other_query,
    one_key,
    other_key,
    one_value,
    other_value,
    mix_share,
    norm_train,
    norm_step,
):
    depth, span = one_key.shape
    wide = one_query.shape[1]
    parts = wide // span
    chips = ranks // CORES
    group = ranks * widths
    bit = norm_train.shape[0]
    late = LATE * span
    tall = -(-depth // LANES) * LANES
    mix_row = mix_share[None]
    if tall != depth:
        mix_row = jnp.pad(mix_row, ((0, 0), (0, tall - depth)))
    shape = jax.ShapeDtypeStruct
    anywhere = pl.BlockSpec(memory_space=pl.ANY)
    near = pl.BlockSpec(memory_space=pltpu.VMEM)
    dma = pltpu.SemaphoreType.DMA
    (
        query, key, value, far_query, far_key, far_value,
        scale_query, scale_key, scale_value, norms,
    ) = pl.pallas_call(
        functools.partial(merge, ranks, widths),
        out_shape=(
            shape((ranks * depth, wide), jnp.bfloat16),
            shape((ranks * depth, span), jnp.bfloat16),
            shape((ranks * depth, span), jnp.bfloat16),
            shape((depth, late), jnp.bfloat16),
            shape((depth, span), jnp.bfloat16),
            shape((depth, span), jnp.bfloat16),
            shape((1, wide), jnp.float32),
            shape((1, span), jnp.float32),
            shape((1, span), jnp.float32),
            shape((group, 1, bit), jnp.float32),
        ),
        in_specs=[anywhere] * 6 + [near] * 3,
        out_specs=[anywhere] * 6 + [near] * 4,
        scratch_shapes=[
            pltpu.VMEM((parts + 2, depth, span), jnp.float32),
            pltpu.VMEM((parts + 2, depth, span), jnp.float32),
            pltpu.VMEM((parts + 2, depth, span), jnp.bfloat16),
            pltpu.VMEM((tall, LANES), jnp.float32),
            pltpu.VMEM((parts + 2, ranks, 1, span), jnp.float32),
            dma((2, parts + 2)),
            dma((parts + 2,)),
            dma((LATE + 2,)),
            dma((parts + 2,)),
            dma((parts + 2,)),
            dma,
            dma,
            dma((chips - 1, parts + 2)),
            dma((chips - 1, parts + 2)),
            dma((chips - 1, parts + 2)),
            dma((chips - 1, parts + 2)),
            dma((2 * chips - 1, parts + 2)),
            dma((2 * chips - 1, parts + 2)),
        ],
        compiler_params=pltpu.CompilerParams(
            collective_id=0, has_side_effects=True, vmem_limit_bytes=56 * 2**20
        ),
    )(
        one_query,
        other_query,
        one_key,
        other_key,
        one_value,
        other_value,
        mix_row,
        norm_train[None],
        norm_step[None],
    )
    ends = (0, chips - 1)
    out = [
        (near * CORES + c, end * CORES + c)
        for near, end in ((1, 0), (chips - 2, chips - 1))
        for c in range(CORES)
    ]
    across = [(end * CORES + c, end * CORES + 1 - c) for end in ends for c in range(CORES)]

    def last_hop(piece):
        return lax.ppermute(piece, "rows", out)

    def to_side(piece):
        return lax.ppermute(piece, "rows", across)

    got_query = last_hop(far_query)
    got_key = last_hop(far_key)
    got_value = last_hop(far_value)
    new_query, new_value, done = settled(query, value, wide - late)
    small = (
        scale_query[0],
        scale_key[0],
        scale_value[0],
        norms.reshape(-1).astype(jnp.bfloat16),
    )
    got_query, got_key, done = lax.optimization_barrier((got_query, got_key, done))
    side_query, side_key = to_side(got_query), to_side(got_key)
    new_query, new_key = blended(
        ranks, wide - late, new_query, query, key, got_query, side_query, got_key, side_key, done
    )
    got_value, new_query, new_key, small = lax.optimization_barrier(
        (got_value, new_query, new_key, small)
    )
    new_value = placed(ranks, new_value, got_value, to_side(got_value))
    return (new_query, new_key, new_value, *small)


def solution(mesh):
    in_specs = (
        P(("site", "rows"), "width"),
        P(("site", "rows"), "width"),
        P(("site", "rows"), "width"),
        P(("site", "rows"), "width"),
        P(("site", "rows"), "width"),
        P(("site", "rows"), "width"),
        P(("site", "rows")),
        P(("site", "rows", "width")),
        P(("site", "rows", "width")),
    )
    out_specs = (
        P("site", "width"),
        P("site", "width"),
        P("site", "width"),
        P(("site", "width")),
        P(("site", "width")),
        P(("site", "width")),
        P("site"),
    )
    body = functools.partial(shards, mesh.shape["rows"], mesh.shape["width"])

    return jax.shard_map(body, mesh=mesh, in_specs=in_specs, out_specs=out_specs, check_vma=False)
```

```python
import functools

import jax
import jax.numpy as jnp
from jax import lax
from jax.experimental import pallas as pl
from jax.experimental.pallas import tpu as pltpu
from jax.sharding import PartitionSpec as P


MESH = pl.DeviceIdType.MESH
CORES = 2
LANES = 128
LATE = 2
AHEAD = 3
PIECES = 4


def merge(
    ranks,
    widths,
    one_query,
    other_query,
    one_key,
    other_key,
    one_value,
    other_value,
    mix_share,
    norm_train,
    norm_step,
    query,
    key,
    value,
    far_query,
    far_key,
    far_value,
    scale_query,
    scale_key,
    scale_value,
    all_norms,
    one,
    other,
    narrow,
    mix_row,
    mix,
    steps,
    norms,
    scales,
    peaks,
    small_sem,
    load_sem,
    out_sem,
    scale_sem,
    far_sem,
    peak_send,
    peak_recv,
    norm_send,
    norm_recv,
    wide_send,
    wide_recv,
    up_send,
    up_recv,
    down_send,
    down_recv,
    side_send,
    side_recv,
    piece_sems,
):
    depth, span = one_key.shape
    parts = one_query.shape[1] // span
    early = parts - LATE
    chips = ranks // CORES
    me = lax.axis_index("rows")
    across = lax.axis_index("width")
    chip, core = me // CORES, me % CORES
    partner = chip * CORES + 1 - core
    last = early - 1
    block = 32 if depth % 32 == 0 else depth
    late_parts = range(early, parts + 2)

    def is_static(k):
        return isinstance(k, int)

    def loads(k):
        if is_static(k) and k >= parts:
            sources = (one_key, other_key) if k == parts else (one_value, other_value)
        else:
            cut = pl.ds(pl.multiple_of(k * span, span), span)
            sources = one_query.at[:, cut], other_query.at[:, cut]
        return [
            pltpu.make_async_copy(source, target.at[k], load_sem.at[i, k])
            for i, (source, target) in enumerate(zip(sources, (one, other)))
        ]

    def load(k):
        for copy in loads(k):
            copy.start()

    barrier = pltpu.get_barrier_semaphore()

    @pl.loop(1, ranks)
    def _(step):
        to = {"rows": lax.rem(me + step, ranks)}
        pl.semaphore_signal(barrier, inc=1, device_id=to, device_id_type=MESH)

    @pl.loop(1, widths)
    def _(step):
        to = {"width": lax.rem(across + step, widths)}
        pl.semaphore_signal(barrier, inc=1, device_id=to, device_id_type=MESH)

    small = [
        pltpu.make_async_copy(mix_share, mix_row, small_sem.at[0]),
        pltpu.make_async_copy(norm_train, steps.at[0], small_sem.at[1]),
        pltpu.make_async_copy(norm_step, steps.at[1], small_sem.at[2]),
    ]
    for copy in small:
        copy.start()

    pl.loop(0, AHEAD)(load)

    for copy in small:
        copy.wait()
    norms[across, me] = steps[0] + steps[1]

    for i in range(mix_row.shape[0]):
        row = jnp.broadcast_to(mix_row[i : i + 1], (LANES, LANES))
        mix[i * LANES : (i + 1) * LANES] = row.T

    def send_peaks(k):
        @pl.loop(1, ranks)
        def _(step):
            pltpu.make_async_remote_copy(
                src_ref=peaks.at[k, me],
                dst_ref=peaks.at[k, me],
                send_sem=peak_send.at[k],
                recv_sem=peak_recv.at[k],
                device_id={"rows": lax.rem(me + step, ranks)},
                device_id_type=MESH,
            ).start()

    def mixed(k):
        for copy in loads(k):
            copy.wait()
        if is_static(k):
            if k + AHEAD < parts + 2:
                load(k + AHEAD)
        else:

            @pl.when(k + AHEAD < parts)
            def _():
                load(k + AHEAD)

            for tail in (parts, parts + 1):

                @pl.when(k + AHEAD == tail)
                def _():
                    load(tail)

        def step(b, top):
            rows = pl.ds(pl.multiple_of(b * block, block), block)
            share = jnp.concatenate([mix[rows]] * (span // LANES), axis=1)
            whole = share * one[k, rows] + (1.0 - share) * other[k, rows]
            one[k, rows] = whole
            return jnp.maximum(top, jnp.max(jnp.abs(whole).reshape(-1, 8, span), axis=0))

        top = lax.fori_loop(0, depth // block, step, jnp.zeros((8, span), jnp.float32))
        peaks[k, me] = jnp.max(top, axis=0, keepdims=True)

    def is_tail(k):
        return is_static(k) and k >= parts

    def hops(k):
        return chips - 2 if is_static(k) and k >= early else chips - 1

    def slot(k, rank):
        rows = pl.ds(pl.multiple_of(rank * depth, depth), depth)
        if is_tail(k):
            return (key if k == parts else value).at[rows]
        return query.at[rows, pl.ds(pl.multiple_of(k * span, span), span)]

    def send(k, rank, to, send_sem, recv_sem, source=None):
        return pltpu.make_async_remote_copy(
            src_ref=slot(k, rank) if source is None else source,
            dst_ref=slot(k, rank),
            send_sem=send_sem,
            recv_sem=recv_sem,
            device_id={"rows": to},
            device_id_type=MESH,
        )

    def go_up(k, hop, source=None):
        return send(k, me - CORES * hop, me + CORES, up_send.at[hop, k], up_recv.at[hop, k], source)

    def go_down(k, hop, source=None):
        return send(
            k, me + CORES * hop, me - CORES, down_send.at[hop, k], down_recv.at[hop, k], source
        )

    def go_side(k, hop, source=None):
        index = hop + chips - 1
        return send(
            k, me + CORES * hop, partner, side_send.at[index, k], side_recv.at[index, k], source
        )

    def from_side(k, hop):
        index = hop + chips - 1
        return send(
            k, partner + CORES * hop, partner, side_send.at[index, k], side_recv.at[index, k]
        )

    def from_below(k, hop):
        return send(k, me - CORES * (hop + 1), me - CORES, up_send.at[hop, k], up_recv.at[hop, k])

    def from_above(k, hop):
        return send(
            k, me + CORES * (hop + 1), me + CORES, down_send.at[hop, k], down_recv.at[hop, k]
        )

    has_below, has_above = chip >= 1, chip < chips - 1

    def keep(k):
        return pltpu.make_async_copy(narrow.at[k], slot(k, me), out_sem.at[k])

    def keep_scale(k):
        if is_tail(k):
            target = scale_key if k == parts else scale_value
        else:
            target = scale_query.at[:, pl.ds(pl.multiple_of(k * span, span), span)]
        return pltpu.make_async_copy(scales.at[k], target, scale_sem.at[k])

    def scaled(k):
        everyone = peaks.at[k, pl.ds(0, ranks - 1)]
        pltpu.make_async_copy(everyone, everyone, peak_recv.at[k]).wait()
        scale = jnp.max(peaks[k], axis=0)
        scales[k] = scale

        @pl.loop(0, depth // block)
        def _(b):
            rows = pl.ds(pl.multiple_of(b * block, block), block)
            narrow[k, rows] = (one[k, rows] / scale).astype(jnp.bfloat16)

        source = narrow.at[k]

        @pl.when(has_below)
        def _():
            go_down(k, 0, source).start()

        @pl.when(has_above)
        def _():
            go_up(k, 0, source).start()

        go_side(k, 0, source).start()
        keep(k).start()
        keep_scale(k).start()

    lag = min(3, parts)
    pl.loop(0, lag)(mixed)
    pl.semaphore_wait(barrier, ranks + widths - 2)
    pl.loop(0, lag)(send_peaks)

    def advance(k):
        mixed(k)
        send_peaks(k)

    @pl.loop(0, parts - lag)
    def _(k):
        scaled(k)
        advance(k + lag)

    advance(parts)
    advance(parts + 1)

    @pl.loop(1, ranks)
    def _(step):
        pltpu.make_async_remote_copy(
            src_ref=norms.at[across, me],
            dst_ref=norms.at[across, me],
            send_sem=norm_send,
            recv_sem=norm_recv,
            device_id={"rows": lax.rem(me + step, ranks)},
            device_id_type=MESH,
        ).start()

    pl.loop(parts - lag, parts)(scaled)
    scaled(parts)
    scaled(parts + 1)

    others = norms.at[across, pl.ds(0, ranks - 1)]
    pltpu.make_async_copy(others, others, norm_recv).wait()

    @pl.loop(1, widths)
    def _(step):
        pltpu.make_async_remote_copy(
            src_ref=norms.at[across],
            dst_ref=norms.at[across],
            send_sem=wide_send,
            recv_sem=wide_recv,
            device_id={"width": lax.rem(across + step, widths)},
            device_id_type=MESH,
        ).start()

    def far_copy(k, rank):
        if is_tail(k):
            target = far_key if k == parts else far_value
        else:
            target = far_query.at[:, pl.ds((k - early) * span, span)]
        return pltpu.make_async_copy(slot(k, rank), target, far_sem.at[k - early])

    def piece(i, to, rank, kind):
        rows = pl.ds(i * (depth // PIECES), depth // PIECES)
        ref = slot(last, rank).at[rows]
        return pltpu.make_async_remote_copy(
            src_ref=ref,
            dst_ref=ref,
            send_sem=piece_sems.at[2 * kind, i],
            recv_sem=piece_sems.at[2 * kind + 1, i],
            device_id={"rows": to},
            device_id_type=MESH,
        )

    reach = CORES * (chips - 1)

    def piece_up(i):
        return piece(i, me + CORES, me + CORES - reach, 0)

    def piece_down(i):
        return piece(i, me - CORES, me - CORES + reach, 0)

    def each_piece(body):
        for i in range(PIECES):
            body(i)

    def last_hop(rank):
        def body(i):
            piece(i, partner, rank, 0).wait_recv()
            piece(i, partner, rank, 1).start()

        each_piece(body)

    def relay(k, hop):
        is_far = is_static(k) and k >= early
        is_last = is_static(k) and k == last
        onward = hop < (chips - 2 if is_last else hops(k))

        @pl.when(chip >= hop)
        def _():
            from_below(k, hop - 1).wait_recv()

            @pl.when(has_above & onward)
            def _():
                go_up(k, hop).start()

            go_side(k, -hop).start()

            if is_last:

                @pl.when((hop == chips - 2) & has_above)
                def _():
                    each_piece(lambda i: piece_up(i).start())

            if is_far:

                @pl.when((hop == chips - 2) & (chip == chips - 2))
                def _():
                    far_copy(k, me - CORES * hop).start()

        @pl.when(chip + hop < chips)
        def _():
            from_above(k, hop - 1).wait_recv()

            @pl.when(has_below & onward)
            def _():
                go_down(k, hop).start()

            go_side(k, hop).start()

            if is_last:

                @pl.when((hop == chips - 2) & has_below)
                def _():
                    each_piece(lambda i: piece_down(i).start())

            if is_far:

                @pl.when((hop == chips - 2) & (chip == 1))
                def _():
                    far_copy(k, me + CORES * hop).start()

    @pl.loop(1, chips - 1)
    def _(hop):
        pl.loop(0, last)(lambda k: relay(k, hop))
        relay(last, hop)
        for k in late_parts:
            relay(k, hop)

    def finish(k):
        keep(k).wait()
        keep_scale(k).wait()
        most = chips - 2 if is_static(k) else chips - 1

        @pl.loop(0, most)
        def _(hop):
            @pl.when((chip >= hop) & has_above)
            def _():
                go_up(k, hop).wait_send()

            @pl.when((chip + hop < chips) & has_below)
            def _():
                go_down(k, hop).wait_send()

        @pl.loop(0, chips)
        def _(origin):
            @pl.when((origin - chip <= most) & (chip - origin <= most))
            def _():
                go_side(k, origin - chip).wait_send()
                from_side(k, origin - chip).wait_recv()

    def settle(k):
        everyone = peaks.at[k, pl.ds(0, ranks - 1)]
        pltpu.make_async_copy(everyone, everyone, peak_send.at[k]).wait()

    for k in late_parts:
        finish(k)

        @pl.when((chip == 1) | (chip == chips - 2))
        def _():
            far_copy(k, me).wait()

    finish(last)
    pl.loop(0, parts + 2)(settle)
    pltpu.make_async_copy(others, others, norm_send).wait()
    around = norms.at[pl.ds(0, widths - 1)]
    pltpu.make_async_copy(around, around, wide_recv).wait()
    pltpu.make_async_copy(around, around, wide_send).wait()
    keep_norms = pltpu.make_async_copy(norms, all_norms, small_sem.at[3])
    keep_norms.start()
    keep_norms.wait()

    @pl.loop(0, last)
    def _(k):
        relay(k, chips - 1)

        @pl.when(k > 0)
        def _():
            finish(k - 1)

    if last > 0:
        finish(jnp.int32(last - 1))

    @pl.when(chip == chips - 1)
    def _():
        last_hop(me - reach)

    @pl.when(chip == 0)
    def _():
        last_hop(me + reach)

    @pl.when((chip == 0) | (chip == chips - 1))
    def _():
        def body(i):
            piece(i, partner, me, 1).wait_send()
            piece(i, partner, me, 1).wait_recv()

        each_piece(body)

    @pl.when((chip == 1) | (chip == chips - 2))
    def _():
        each_piece(lambda i: piece(i, partner, me, 0).wait_send())


def stream(total, incoming, outgoing, ring):
    ahead = ring // 2

    def head():
        for i in range(min(ahead, total)):
            incoming(i, True)

    def body():
        @pl.loop(0, total)
        def _(i):
            incoming(i, False)
            outgoing(i).start()

            @pl.when(i + ahead < total)
            def _():
                @pl.when(i + ahead >= ring)
                def _():
                    outgoing(i + ahead - ring).wait()

                incoming(i + ahead, True)

    def drain():
        @pl.loop(max(0, total - ring), total)
        def _(i):
            outgoing(i).wait()

    return head, body, drain


def act(copy, begin):
    if begin:
        copy.start()
    else:
        copy.wait()


def settle_kernel(
    query,
    value,
    scale_key,
    scale_value,
    new_query,
    new_value,
    new_scale_key,
    new_scale_value,
    done,
    wide_buf,
    slim_buf,
    sems,
):
    ring = wide_buf.shape[0]

    def plan(source, target, buf, at):
        step = buf.shape[1]
        cols = pl.ds(0, buf.shape[2])

        def rows(i):
            return pl.ds(pl.multiple_of(i * step, step), step)

        def incoming(i, begin):
            place = lax.rem(i, ring)
            act(
                pltpu.make_async_copy(
                    source.at[rows(i), cols], buf.at[place], sems.at[at, place]
                ),
                begin,
            )

        def outgoing(i):
            place = lax.rem(i, ring)
            return pltpu.make_async_copy(
                buf.at[place], target.at[rows(i), cols], sems.at[at + 1, place]
            )

        return stream(source.shape[0] // step, incoming, outgoing, ring)

    first = plan(query, new_query, wide_buf, 0)
    second = plan(value, new_value, slim_buf, 2)
    first[0]()
    first[1]()
    second[0]()
    second[1]()
    first[2]()
    second[2]()
    new_scale_key[...] = scale_key[...]
    new_scale_value[...] = scale_value[...]
    done[...] = jnp.zeros_like(done)


def chunk_of(rows, most):
    step = rows
    while step > most and step % 32 == 0:
        step //= 2
    return step


def settled(query, value, scale_key, scale_value, wide, ring=8):
    rows, span = value.shape
    step = chunk_of(rows, 128)
    slim = chunk_of(rows, 512)
    anywhere = pl.BlockSpec(memory_space=pl.ANY)
    near = pl.BlockSpec(memory_space=pltpu.VMEM)
    moved = 4 * rows * (wide + span)
    return pl.pallas_call(
        settle_kernel,
        out_shape=(
            jax.ShapeDtypeStruct(query.shape, query.dtype),
            jax.ShapeDtypeStruct(value.shape, value.dtype),
            jax.ShapeDtypeStruct(scale_key.shape, scale_key.dtype),
            jax.ShapeDtypeStruct(scale_value.shape, scale_value.dtype),
            jax.ShapeDtypeStruct((8, LANES), jnp.float32),
        ),
        in_specs=[anywhere, anywhere, near, near],
        out_specs=(anywhere, anywhere, near, near, near),
        scratch_shapes=[
            pltpu.VMEM((ring, step, wide), query.dtype),
            pltpu.VMEM((ring, slim, span), value.dtype),
            pltpu.SemaphoreType.DMA((4, ring)),
        ],
        compiler_params=pltpu.CompilerParams(vmem_limit_bytes=60 * 2**20),
        cost_estimate=pl.CostEstimate(
            flops=0, bytes_accessed=moved, transcendentals=0
        ),
    )(query, value, scale_key, scale_value)


def far_ranks(ranks):
    chips = ranks // CORES
    me = lax.axis_index("rows")
    chip, core = me // CORES, me % CORES
    at_end = (chip == 0) | (chip == chips - 1)
    away = jnp.where(chip == 0, chips - 1, 0) * CORES
    return at_end, away + core, away + 1 - core


def blend_kernel(ranks, first, fresh, whole, got, side, done, target, buf, sems):
    at_end, straight, crossed = far_ranks(ranks)
    ring, depth, span = buf.shape
    cols = pl.ds(first, span)

    def rows(i):
        return pl.ds(pl.multiple_of(i * depth, depth), depth)

    def incoming(i, begin):
        place = lax.rem(i, ring)

        def copy(origin):
            act(pltpu.make_async_copy(origin, buf.at[place], sems.at[0, place]), begin)

        if not begin:
            copy(whole.at[rows(i), cols])
            return
        is_got = at_end & (i == straight)
        is_side = at_end & (i == crossed)
        pl.when(is_got)(lambda: copy(got))
        pl.when(is_side)(lambda: copy(side))
        pl.when(jnp.logical_not(is_got | is_side))(lambda: copy(whole.at[rows(i), cols]))

    def outgoing(i):
        place = lax.rem(i, ring)
        return pltpu.make_async_copy(buf.at[place], target.at[rows(i), cols], sems.at[1, place])

    for phase in stream(ranks, incoming, outgoing, ring):
        phase()


def blended(ranks, first, fresh, whole, got, side, done, ring=6):
    anywhere = pl.BlockSpec(memory_space=pl.ANY)
    return pl.pallas_call(
        functools.partial(blend_kernel, ranks, first),
        out_shape=jax.ShapeDtypeStruct(whole.shape, whole.dtype),
        in_specs=[anywhere] * 5,
        out_specs=anywhere,
        scratch_shapes=[
            pltpu.VMEM((ring, *got.shape), whole.dtype),
            pltpu.SemaphoreType.DMA((2, ring)),
        ],
        input_output_aliases={} if fresh is done else {0: 0},
        compiler_params=pltpu.CompilerParams(vmem_limit_bytes=60 * 2**20),
        cost_estimate=pl.CostEstimate(
            flops=0, bytes_accessed=4 * ranks * got.size, transcendentals=0
        ),
    )(fresh, whole, got, side, done)


def place_kernel(ranks, _, got, side, target, sems):
    at_end, straight, crossed = far_ranks(ranks)
    depth = got.shape[0]

    @pl.when(at_end)
    def _():
        copies = [
            pltpu.make_async_copy(
                source, target.at[pl.ds(pl.multiple_of(rank * depth, depth), depth)], sems.at[i]
            )
            for i, (source, rank) in enumerate(((got, straight), (side, crossed)))
        ]
        for copy in copies:
            copy.start()
        for copy in copies:
            copy.wait()


def placed(ranks, whole, got, side):
    anywhere = pl.BlockSpec(memory_space=pl.ANY)
    near = pl.BlockSpec(memory_space=pltpu.VMEM)
    return pl.pallas_call(
        functools.partial(place_kernel, ranks),
        out_shape=jax.ShapeDtypeStruct(whole.shape, whole.dtype),
        in_specs=[anywhere, near, near],
        out_specs=anywhere,
        scratch_shapes=[pltpu.SemaphoreType.DMA((2,))],
        input_output_aliases={0: 0},
        compiler_params=pltpu.CompilerParams(vmem_limit_bytes=8 * 2**20),
        cost_estimate=pl.CostEstimate(
            flops=0, bytes_accessed=4 * got.size, transcendentals=0
        ),
    )(whole, got, side)


def shards(
    ranks,
    widths,
    one_query,
    other_query,
    one_key,
    other_key,
    one_value,
    other_value,
    mix_share,
    norm_train,
    norm_step,
):
    depth, span = one_key.shape
    wide = one_query.shape[1]
    parts = wide // span
    chips = ranks // CORES
    bit = norm_train.shape[0]
    late = LATE * span
    tall = -(-depth // LANES) * LANES
    if tall != depth:
        mix_share = jnp.pad(mix_share, (0, tall - depth))
    mix_rows = mix_share.reshape(tall // LANES, LANES)
    shape = jax.ShapeDtypeStruct
    anywhere = pl.BlockSpec(memory_space=pl.ANY)
    dma = pltpu.SemaphoreType.DMA
    (
        query, key, value, far_query, far_key, far_value,
        scale_query, scale_key, scale_value, norms,
    ) = pl.pallas_call(
        functools.partial(merge, ranks, widths),
        out_shape=(
            shape((ranks * depth, wide), jnp.bfloat16),
            shape((ranks * depth, span), jnp.bfloat16),
            shape((ranks * depth, span), jnp.bfloat16),
            shape((depth, late), jnp.bfloat16),
            shape((depth, span), jnp.bfloat16),
            shape((depth, span), jnp.bfloat16),
            shape((1, wide), jnp.float32),
            shape((1, span), jnp.float32),
            shape((1, span), jnp.float32),
            shape((widths, ranks, 1, bit), jnp.float32),
        ),
        in_specs=[anywhere] * 9,
        out_specs=[anywhere] * 10,
        scratch_shapes=[
            pltpu.VMEM((parts + 2, depth, span), jnp.float32),
            pltpu.VMEM((parts + 2, depth, span), jnp.float32),
            pltpu.VMEM((parts + 2, depth, span), jnp.bfloat16),
            pltpu.VMEM(mix_rows.shape, jnp.float32),
            pltpu.VMEM((tall, LANES), jnp.float32),
            pltpu.VMEM((2, 1, bit), jnp.float32),
            pltpu.VMEM((widths, ranks, 1, bit), jnp.float32),
            pltpu.VMEM((parts + 2, 1, span), jnp.float32),
            pltpu.VMEM((parts + 2, ranks, 1, span), jnp.float32),
            dma((4,)),
            dma((2, parts + 2)),
            dma((parts + 2,)),
            dma((parts + 2,)),
            dma((LATE + 2,)),
            dma((parts + 2,)),
            dma((parts + 2,)),
            dma,
            dma,
            dma,
            dma,
            dma((chips - 1, parts + 2)),
            dma((chips - 1, parts + 2)),
            dma((chips - 1, parts + 2)),
            dma((chips - 1, parts + 2)),
            dma((2 * chips - 1, parts + 2)),
            dma((2 * chips - 1, parts + 2)),
            dma((4, PIECES)),
        ],
        compiler_params=pltpu.CompilerParams(
            collective_id=0, has_side_effects=True, vmem_limit_bytes=56 * 2**20
        ),
    )(
        one_query,
        other_query,
        one_key,
        other_key,
        one_value,
        other_value,
        mix_rows,
        norm_train[None],
        norm_step[None],
    )
    ends = (0, chips - 1)
    out = [
        (near * CORES + c, end * CORES + c)
        for near, end in ((1, 0), (chips - 2, chips - 1))
        for c in range(CORES)
    ]
    across = [(end * CORES + c, end * CORES + 1 - c) for end in ends for c in range(CORES)]

    def last_hop(piece):
        return lax.ppermute(piece, "rows", out)

    def to_side(piece):
        return lax.ppermute(piece, "rows", across)

    got_query = last_hop(far_query)
    got_key = last_hop(far_key)
    got_value = last_hop(far_value)
    new_query, new_value, scale_key, scale_value, done = settled(
        query, value, scale_key, scale_value, wide - late
    )
    small = (
        scale_query[0],
        scale_key[0],
        scale_value[0],
        norms.transpose(1, 0, 2, 3).reshape(-1).astype(jnp.bfloat16),
    )
    got_query, done = lax.optimization_barrier((got_query, done))
    new_query = blended(
        ranks, wide - late, new_query, query, got_query, to_side(got_query), done
    )
    got_key, new_query = lax.optimization_barrier((got_key, new_query))
    new_key = blended(ranks, 0, done, key, got_key, to_side(got_key), done)
    got_value, new_key, small = lax.optimization_barrier((got_value, new_key, small))
    new_value = placed(ranks, new_value, got_value, to_side(got_value))
    return (new_query, new_key, new_value, *small)


def solution(mesh):
    in_specs = (
        P(("site", "rows"), "width"),
        P(("site", "rows"), "width"),
        P(("site", "rows"), "width"),
        P(("site", "rows"), "width"),
        P(("site", "rows"), "width"),
        P(("site", "rows"), "width"),
        P(("site", "rows")),
        P(("site", "rows", "width")),
        P(("site", "rows", "width")),
    )
    out_specs = (
        P("site", "width"),
        P("site", "width"),
        P("site", "width"),
        P(("site", "width")),
        P(("site", "width")),
        P(("site", "width")),
        P("site"),
    )
    body = functools.partial(shards, mesh.shape["rows"], mesh.shape["width"])

    return jax.shard_map(
        body, mesh=mesh, in_specs=in_specs, out_specs=out_specs, check_vma=False
    )
```

```python
import functools

import jax
import jax.numpy as jnp
from jax import lax
from jax.experimental import pallas as pl
from jax.experimental.pallas import tpu as pltpu
from jax.sharding import PartitionSpec as P


MESH = pl.DeviceIdType.MESH
CORES = 2
LANES = 128
LATE = 2
AHEAD = 3


def merge(
    ranks,
    widths,
    one_query,
    other_query,
    one_key,
    other_key,
    one_value,
    other_value,
    mix_share,
    norm_train,
    norm_step,
    query,
    key,
    value,
    far_early,
    far_query,
    far_key,
    far_value,
    scale_query,
    scale_key,
    scale_value,
    all_norms,
    one,
    other,
    narrow,
    mix_row,
    mix,
    steps,
    norms,
    scales,
    peaks,
    small_sem,
    load_sem,
    out_sem,
    scale_sem,
    far_sem,
    peak_send,
    peak_recv,
    norm_send,
    norm_recv,
    wide_send,
    wide_recv,
    up_send,
    up_recv,
    down_send,
    down_recv,
    side_send,
    side_recv,
    early_send,
    early_recv,
):
    depth, span = one_key.shape
    parts = one_query.shape[1] // span
    early = parts - LATE
    chips = ranks // CORES
    me = lax.axis_index("rows")
    across = lax.axis_index("width")
    chip, core = me // CORES, me % CORES
    partner = chip * CORES + 1 - core
    last = early - 1
    block = 32 if depth % 32 == 0 else depth
    late_parts = range(early, parts + 2)

    def is_static(k):
        return isinstance(k, int)

    def loads(k):
        if is_static(k) and k >= parts:
            sources = (one_key, other_key) if k == parts else (one_value, other_value)
        else:
            cut = pl.ds(pl.multiple_of(k * span, span), span)
            sources = one_query.at[:, cut], other_query.at[:, cut]
        return [
            pltpu.make_async_copy(source, target.at[k], load_sem.at[i, k])
            for i, (source, target) in enumerate(zip(sources, (one, other)))
        ]

    def load(k):
        for copy in loads(k):
            copy.start()

    barrier = pltpu.get_barrier_semaphore()

    @pl.loop(1, ranks)
    def _(step):
        to = {"rows": lax.rem(me + step, ranks)}
        pl.semaphore_signal(barrier, inc=1, device_id=to, device_id_type=MESH)

    @pl.loop(1, widths)
    def _(step):
        to = {"width": lax.rem(across + step, widths)}
        pl.semaphore_signal(barrier, inc=1, device_id=to, device_id_type=MESH)

    small = [
        pltpu.make_async_copy(mix_share, mix_row, small_sem.at[0]),
        pltpu.make_async_copy(norm_train, steps.at[0], small_sem.at[1]),
        pltpu.make_async_copy(norm_step, steps.at[1], small_sem.at[2]),
    ]
    for copy in small:
        copy.start()

    pl.loop(0, AHEAD)(load)

    for copy in small:
        copy.wait()
    norms[across, me] = steps[0] + steps[1]

    for i in range(mix_row.shape[0]):
        row = jnp.broadcast_to(mix_row[i : i + 1], (LANES, LANES))
        mix[i * LANES : (i + 1) * LANES] = row.T

    def send_peaks(k):
        @pl.loop(1, ranks)
        def _(step):
            pltpu.make_async_remote_copy(
                src_ref=peaks.at[k, me],
                dst_ref=peaks.at[k, me],
                send_sem=peak_send.at[k],
                recv_sem=peak_recv.at[k],
                device_id={"rows": lax.rem(me + step, ranks)},
                device_id_type=MESH,
            ).start()

    def mixed(k):
        for copy in loads(k):
            copy.wait()
        if is_static(k):
            if k + AHEAD < parts + 2:
                load(k + AHEAD)
        else:

            @pl.when(k + AHEAD < parts)
            def _():
                load(k + AHEAD)

            for tail in (parts, parts + 1):

                @pl.when(k + AHEAD == tail)
                def _():
                    load(tail)

        def step(b, top):
            rows = pl.ds(pl.multiple_of(b * block, block), block)
            share = jnp.concatenate([mix[rows]] * (span // LANES), axis=1)
            whole = share * one[k, rows] + (1.0 - share) * other[k, rows]
            one[k, rows] = whole
            return jnp.maximum(top, jnp.max(jnp.abs(whole).reshape(-1, 8, span), axis=0))

        top = lax.fori_loop(0, depth // block, step, jnp.zeros((8, span), jnp.float32))
        peaks[k, me] = jnp.max(top, axis=0, keepdims=True)

    def is_tail(k):
        return is_static(k) and k >= parts

    def hops(k):
        return chips - 2 if is_static(k) and k >= early else chips - 1

    def slot(k, rank):
        rows = pl.ds(pl.multiple_of(rank * depth, depth), depth)
        if is_tail(k):
            return (key if k == parts else value).at[rows]
        return query.at[rows, pl.ds(pl.multiple_of(k * span, span), span)]

    def send(k, rank, to, send_sem, recv_sem, source=None):
        return pltpu.make_async_remote_copy(
            src_ref=slot(k, rank) if source is None else source,
            dst_ref=slot(k, rank),
            send_sem=send_sem,
            recv_sem=recv_sem,
            device_id={"rows": to},
            device_id_type=MESH,
        )

    def go_up(k, hop, source=None):
        return send(k, me - CORES * hop, me + CORES, up_send.at[hop, k], up_recv.at[hop, k], source)

    def go_down(k, hop, source=None):
        return send(
            k, me + CORES * hop, me - CORES, down_send.at[hop, k], down_recv.at[hop, k], source
        )

    def go_side(k, hop, source=None):
        index = hop + chips - 1
        return send(
            k, me + CORES * hop, partner, side_send.at[index, k], side_recv.at[index, k], source
        )

    def from_side(k, hop):
        index = hop + chips - 1
        return send(
            k, partner + CORES * hop, partner, side_send.at[index, k], side_recv.at[index, k]
        )

    def from_below(k, hop):
        return send(k, me - CORES * (hop + 1), me - CORES, up_send.at[hop, k], up_recv.at[hop, k])

    def from_above(k, hop):
        return send(
            k, me + CORES * (hop + 1), me + CORES, down_send.at[hop, k], down_recv.at[hop, k]
        )

    has_below, has_above = chip >= 1, chip < chips - 1

    def keep(k):
        return pltpu.make_async_copy(narrow.at[k], slot(k, me), out_sem.at[k])

    def keep_scale(k):
        if is_tail(k):
            target = scale_key if k == parts else scale_value
        else:
            target = scale_query.at[:, pl.ds(pl.multiple_of(k * span, span), span)]
        return pltpu.make_async_copy(scales.at[k], target, scale_sem.at[k])

    def scaled(k):
        everyone = peaks.at[k, pl.ds(0, ranks - 1)]
        pltpu.make_async_copy(everyone, everyone, peak_recv.at[k]).wait()
        scale = jnp.max(peaks[k], axis=0)
        scales[k] = scale

        @pl.loop(0, depth // block)
        def _(b):
            rows = pl.ds(pl.multiple_of(b * block, block), block)
            narrow[k, rows] = (one[k, rows] / scale).astype(jnp.bfloat16)

        source = narrow.at[k]

        @pl.when(has_below)
        def _():
            go_down(k, 0, source).start()

        @pl.when(has_above)
        def _():
            go_up(k, 0, source).start()

        go_side(k, 0, source).start()
        keep(k).start()
        keep_scale(k).start()

    lag = min(3, parts)
    pl.loop(0, lag)(mixed)
    pl.semaphore_wait(barrier, ranks + widths - 2)
    pl.loop(0, lag)(send_peaks)

    def advance(k):
        mixed(k)
        send_peaks(k)

    @pl.loop(0, parts - lag)
    def _(k):
        scaled(k)
        advance(k + lag)

    advance(parts)
    advance(parts + 1)

    @pl.loop(1, ranks)
    def _(step):
        pltpu.make_async_remote_copy(
            src_ref=norms.at[across, me],
            dst_ref=norms.at[across, me],
            send_sem=norm_send,
            recv_sem=norm_recv,
            device_id={"rows": lax.rem(me + step, ranks)},
            device_id_type=MESH,
        ).start()

    pl.loop(parts - lag, parts)(scaled)
    scaled(parts)
    scaled(parts + 1)

    others = norms.at[across, pl.ds(0, ranks - 1)]
    pltpu.make_async_copy(others, others, norm_recv).wait()

    @pl.loop(1, widths)
    def _(step):
        pltpu.make_async_remote_copy(
            src_ref=norms.at[across],
            dst_ref=norms.at[across],
            send_sem=wide_send,
            recv_sem=wide_recv,
            device_id={"width": lax.rem(across + step, widths)},
            device_id_type=MESH,
        ).start()

    def far_copy(k, rank):
        if is_tail(k):
            target = far_key if k == parts else far_value
        elif k == last:
            target = far_early
        else:
            target = far_query.at[:, pl.ds((k - early) * span, span)]
        return pltpu.make_async_copy(slot(k, rank), target, far_sem.at[k - last])

    def last_early(rank, to):
        return pltpu.make_async_remote_copy(
            src_ref=slot(last, rank),
            dst_ref=far_early,
            send_sem=early_send,
            recv_sem=early_recv,
            device_id={"rows": to},
            device_id_type=MESH,
        )

    def relay(k, hop):
        is_far = is_static(k)
        is_last = is_static(k) and k == last
        onward = hop < (chips - 2 if is_last else hops(k))

        @pl.when(chip >= hop)
        def _():
            from_below(k, hop - 1).wait_recv()

            @pl.when(has_above & onward)
            def _():
                go_up(k, hop).start()

            go_side(k, -hop).start()

            if is_last:

                @pl.when((hop == chips - 2) & has_above & (core == 1))
                def _():
                    last_early(me - CORES * hop, me + CORES).start()

            if is_far:

                @pl.when((hop == chips - 2) & (chip == chips - 2))
                def _():
                    far_copy(k, me - CORES * hop).start()

        @pl.when(chip + hop < chips)
        def _():
            from_above(k, hop - 1).wait_recv()

            @pl.when(has_below & onward)
            def _():
                go_down(k, hop).start()

            go_side(k, hop).start()

            if is_last:

                @pl.when((hop == chips - 2) & has_below & (core == 1))
                def _():
                    last_early(me + CORES * hop, me - CORES).start()

            if is_far:

                @pl.when((hop == chips - 2) & (chip == 1))
                def _():
                    far_copy(k, me + CORES * hop).start()

    @pl.loop(1, chips - 1)
    def _(hop):
        pl.loop(0, last)(lambda k: relay(k, hop))
        relay(last, hop)
        for k in late_parts:
            relay(k, hop)

    def finish(k):
        keep(k).wait()
        keep_scale(k).wait()
        most = chips - 2 if is_static(k) else chips - 1

        @pl.loop(0, most)
        def _(hop):
            @pl.when((chip >= hop) & has_above)
            def _():
                go_up(k, hop).wait_send()

            @pl.when((chip + hop < chips) & has_below)
            def _():
                go_down(k, hop).wait_send()

        @pl.loop(0, chips)
        def _(origin):
            @pl.when((origin - chip <= most) & (chip - origin <= most))
            def _():
                go_side(k, origin - chip).wait_send()
                from_side(k, origin - chip).wait_recv()

    def settle(k):
        everyone = peaks.at[k, pl.ds(0, ranks - 1)]
        pltpu.make_async_copy(everyone, everyone, peak_send.at[k]).wait()

    near_end = (chip == 1) | (chip == chips - 2)
    at_end = (chip == 0) | (chip == chips - 1)

    for k in (last, *late_parts):
        finish(k)

        @pl.when(near_end)
        def _():
            far_copy(k, me).wait()

    pl.loop(0, parts + 2)(settle)
    pltpu.make_async_copy(others, others, norm_send).wait()
    around = norms.at[pl.ds(0, widths - 1)]
    pltpu.make_async_copy(around, around, wide_recv).wait()
    pltpu.make_async_copy(around, around, wide_send).wait()
    keep_norms = pltpu.make_async_copy(norms, all_norms, small_sem.at[3])
    keep_norms.start()
    keep_norms.wait()

    @pl.loop(0, last)
    def _(k):
        relay(k, chips - 1)

        @pl.when(k > 0)
        def _():
            finish(k - 1)

    if last > 0:
        finish(jnp.int32(last - 1))

    @pl.when(at_end & (core == 1))
    def _():
        last_early(me, partner).wait_recv()

    @pl.when(near_end & (core == 1))
    def _():
        last_early(me, partner).wait_send()


def stream(total, incoming, outgoing, ring):
    ahead = ring // 2

    def head():
        for i in range(min(ahead, total)):
            incoming(i, True)

    def body():
        @pl.loop(0, total)
        def _(i):
            incoming(i, False)
            outgoing(i).start()

            @pl.when(i + ahead < total)
            def _():
                @pl.when(i + ahead >= ring)
                def _():
                    outgoing(i + ahead - ring).wait()

                incoming(i + ahead, True)

    def drain():
        @pl.loop(max(0, total - ring), total)
        def _(i):
            outgoing(i).wait()

    return head, body, drain


def act(copy, begin):
    if begin:
        copy.start()
    else:
        copy.wait()


def settle_kernel(
    query,
    value,
    scale_key,
    scale_value,
    new_query,
    new_value,
    new_scale_key,
    new_scale_value,
    done,
    wide_buf,
    slim_buf,
    sems,
):
    ring = wide_buf.shape[0]

    def plan(source, target, buf, at):
        step = buf.shape[1]
        cols = pl.ds(0, buf.shape[2])

        def rows(i):
            return pl.ds(pl.multiple_of(i * step, step), step)

        def incoming(i, begin):
            place = lax.rem(i, ring)
            act(
                pltpu.make_async_copy(
                    source.at[rows(i), cols], buf.at[place], sems.at[at, place]
                ),
                begin,
            )

        def outgoing(i):
            place = lax.rem(i, ring)
            return pltpu.make_async_copy(
                buf.at[place], target.at[rows(i), cols], sems.at[at + 1, place]
            )

        return stream(source.shape[0] // step, incoming, outgoing, ring)

    first = plan(query, new_query, wide_buf, 0)
    second = plan(value, new_value, slim_buf, 2)
    first[0]()
    first[1]()
    second[0]()
    second[1]()
    first[2]()
    second[2]()
    new_scale_key[...] = scale_key[...]
    new_scale_value[...] = scale_value[...]
    done[...] = jnp.zeros_like(done)


def chunk_of(rows, most):
    step = rows
    while step > most and step % 32 == 0:
        step //= 2
    return step


def settled(query, value, scale_key, scale_value, wide, ring=8):
    rows, span = value.shape
    step = chunk_of(rows, 256)
    slim = chunk_of(rows, 512)
    anywhere = pl.BlockSpec(memory_space=pl.ANY)
    near = pl.BlockSpec(memory_space=pltpu.VMEM)
    moved = 4 * rows * (wide + span)
    return pl.pallas_call(
        settle_kernel,
        out_shape=(
            jax.ShapeDtypeStruct(query.shape, query.dtype),
            jax.ShapeDtypeStruct(value.shape, value.dtype),
            jax.ShapeDtypeStruct(scale_key.shape, scale_key.dtype),
            jax.ShapeDtypeStruct(scale_value.shape, scale_value.dtype),
            jax.ShapeDtypeStruct((8, LANES), jnp.float32),
        ),
        in_specs=[anywhere, anywhere, near, near],
        out_specs=(anywhere, anywhere, near, near, near),
        scratch_shapes=[
            pltpu.VMEM((ring, step, wide), query.dtype),
            pltpu.VMEM((ring, slim, span), value.dtype),
            pltpu.SemaphoreType.DMA((4, ring)),
        ],
        compiler_params=pltpu.CompilerParams(vmem_limit_bytes=60 * 2**20),
        cost_estimate=pl.CostEstimate(
            flops=0, bytes_accessed=moved, transcendentals=0
        ),
    )(query, value, scale_key, scale_value)


def far_ranks(ranks):
    chips = ranks // CORES
    me = lax.axis_index("rows")
    chip, core = me // CORES, me % CORES
    at_end = (chip == 0) | (chip == chips - 1)
    away = jnp.where(chip == 0, chips - 1, 0) * CORES
    return at_end, away + core, away + 1 - core


def blend_kernel(ranks, first, fresh, whole, got0, got1, side0, side1, done, target, buf, sems):
    at_end, straight, crossed = far_ranks(ranks)
    core = lax.axis_index("rows") % CORES
    ring, depth, span = buf.shape
    cols = pl.ds(first, span)

    def rows(i):
        return pl.ds(pl.multiple_of(i * depth, depth), depth)

    def incoming(i, begin):
        place = lax.rem(i, ring)

        def copy(origin):
            act(pltpu.make_async_copy(origin, buf.at[place], sems.at[0, place]), begin)

        if not begin:
            copy(whole.at[rows(i), cols])
            return
        is_got = at_end & (i == straight)
        is_side = at_end & (i == crossed)
        pl.when(is_got & (core == 0))(lambda: copy(got0))
        pl.when(is_got & (core == 1))(lambda: copy(got1))
        pl.when(is_side & (core == 0))(lambda: copy(side0))
        pl.when(is_side & (core == 1))(lambda: copy(side1))
        pl.when(jnp.logical_not(is_got | is_side))(lambda: copy(whole.at[rows(i), cols]))

    def outgoing(i):
        place = lax.rem(i, ring)
        return pltpu.make_async_copy(
            buf.at[place], target.at[rows(i), cols], sems.at[1, place]
        )

    for phase in stream(ranks, incoming, outgoing, ring):
        phase()


def blended(ranks, first, fresh, whole, gots, sides, done, ring=6):
    anywhere = pl.BlockSpec(memory_space=pl.ANY)
    return pl.pallas_call(
        functools.partial(blend_kernel, ranks, first),
        out_shape=jax.ShapeDtypeStruct(whole.shape, whole.dtype),
        in_specs=[anywhere] * 7,
        out_specs=anywhere,
        scratch_shapes=[
            pltpu.VMEM((ring, *gots[0].shape), whole.dtype),
            pltpu.SemaphoreType.DMA((2, ring)),
        ],
        input_output_aliases={} if fresh is done else {0: 0},
        compiler_params=pltpu.CompilerParams(vmem_limit_bytes=60 * 2**20),
        cost_estimate=pl.CostEstimate(
            flops=0, bytes_accessed=4 * ranks * gots[0].size, transcendentals=0
        ),
    )(fresh, whole, *gots, *sides, done)


def place_kernel(ranks, _, got, side, target, sems):
    at_end, straight, crossed = far_ranks(ranks)
    depth = got.shape[0]

    @pl.when(at_end)
    def _():
        copies = [
            pltpu.make_async_copy(
                source, target.at[pl.ds(pl.multiple_of(rank * depth, depth), depth)], sems.at[i]
            )
            for i, (source, rank) in enumerate(((got, straight), (side, crossed)))
        ]
        for copy in copies:
            copy.start()
        for copy in copies:
            copy.wait()


def placed(ranks, whole, got, side):
    anywhere = pl.BlockSpec(memory_space=pl.ANY)
    near = pl.BlockSpec(memory_space=pltpu.VMEM)
    return pl.pallas_call(
        functools.partial(place_kernel, ranks),
        out_shape=jax.ShapeDtypeStruct(whole.shape, whole.dtype),
        in_specs=[anywhere, near, near],
        out_specs=anywhere,
        scratch_shapes=[pltpu.SemaphoreType.DMA((2,))],
        input_output_aliases={0: 0},
        compiler_params=pltpu.CompilerParams(vmem_limit_bytes=8 * 2**20),
        cost_estimate=pl.CostEstimate(
            flops=0, bytes_accessed=4 * got.size, transcendentals=0
        ),
    )(whole, got, side)


def shards(
    ranks,
    widths,
    one_query,
    other_query,
    one_key,
    other_key,
    one_value,
    other_value,
    mix_share,
    norm_train,
    norm_step,
):
    depth, span = one_key.shape
    wide = one_query.shape[1]
    parts = wide // span
    chips = ranks // CORES
    bit = norm_train.shape[0]
    late = LATE * span
    tall = -(-depth // LANES) * LANES
    if tall != depth:
        mix_share = jnp.pad(mix_share, (0, tall - depth))
    mix_rows = mix_share.reshape(tall // LANES, LANES)
    shape = jax.ShapeDtypeStruct
    anywhere = pl.BlockSpec(memory_space=pl.ANY)
    dma = pltpu.SemaphoreType.DMA
    (
        query, key, value, far_early, far_query, far_key, far_value,
        scale_query, scale_key, scale_value, norms,
    ) = pl.pallas_call(
        functools.partial(merge, ranks, widths),
        out_shape=(
            shape((ranks * depth, wide), jnp.bfloat16),
            shape((ranks * depth, span), jnp.bfloat16),
            shape((ranks * depth, span), jnp.bfloat16),
            shape((depth, span), jnp.bfloat16),
            shape((depth, late), jnp.bfloat16),
            shape((depth, span), jnp.bfloat16),
            shape((depth, span), jnp.bfloat16),
            shape((1, wide), jnp.float32),
            shape((1, span), jnp.float32),
            shape((1, span), jnp.float32),
            shape((widths, ranks, 1, bit), jnp.float32),
        ),
        in_specs=[anywhere] * 9,
        out_specs=[anywhere] * 11,
        scratch_shapes=[
            pltpu.VMEM((parts + 2, depth, span), jnp.float32),
            pltpu.VMEM((parts + 2, depth, span), jnp.float32),
            pltpu.VMEM((parts + 2, depth, span), jnp.bfloat16),
            pltpu.VMEM(mix_rows.shape, jnp.float32),
            pltpu.VMEM((tall, LANES), jnp.float32),
            pltpu.VMEM((2, 1, bit), jnp.float32),
            pltpu.VMEM((widths, ranks, 1, bit), jnp.float32),
            pltpu.VMEM((parts + 2, 1, span), jnp.float32),
            pltpu.VMEM((parts + 2, ranks, 1, span), jnp.float32),
            dma((4,)),
            dma((2, parts + 2)),
            dma((parts + 2,)),
            dma((parts + 2,)),
            dma((LATE + 3,)),
            dma((parts + 2,)),
            dma((parts + 2,)),
            dma,
            dma,
            dma,
            dma,
            dma((chips - 1, parts + 2)),
            dma((chips - 1, parts + 2)),
            dma((chips - 1, parts + 2)),
            dma((chips - 1, parts + 2)),
            dma((2 * chips - 1, parts + 2)),
            dma((2 * chips - 1, parts + 2)),
            dma,
            dma,
        ],
        compiler_params=pltpu.CompilerParams(
            collective_id=0, has_side_effects=True, vmem_limit_bytes=56 * 2**20
        ),
    )(
        one_query,
        other_query,
        one_key,
        other_key,
        one_value,
        other_value,
        mix_rows,
        norm_train[None],
        norm_step[None],
    )
    first = wide - late - span
    ends = ((1, 0), (chips - 2, chips - 1))

    def send(piece, *pairs):
        return lax.ppermute(
            piece,
            "rows",
            [
                (source * CORES + a, target * CORES + b)
                for near, end in ends
                for hop in pairs
                for (source, a), (target, b) in [
                    ((near if hop[0] else end, hop[1]), (end, hop[2]))
                ]
            ],
        )

    def last_hop(piece):
        return send(piece, (True, 0, 0), (True, 1, 1))

    def to_side(piece):
        return send(piece, (False, 0, 1), (False, 1, 0))

    got_early = send(far_early, (True, 0, 0))
    got_query = last_hop(far_query)
    got_key = last_hop(far_key)
    got_value = last_hop(far_value)
    new_query, new_value, scale_key, scale_value, done = settled(
        query, value, scale_key, scale_value, first
    )
    small = (
        scale_query[0],
        scale_key[0],
        scale_value[0],
        norms.transpose(1, 0, 2, 3).reshape(-1).astype(jnp.bfloat16),
    )
    got_early, far_early, done = lax.optimization_barrier((got_early, far_early, done))
    sides = send(far_early, (False, 1, 0)), send(got_early, (False, 0, 1))
    new_query = blended(
        ranks, first, new_query, query, (got_early, far_early), sides, done
    )
    got_query, new_query = lax.optimization_barrier((got_query, new_query))
    new_query = blended(
        ranks, first + span, new_query, query, [got_query] * 2, [to_side(got_query)] * 2, done
    )
    got_key, new_query = lax.optimization_barrier((got_key, new_query))
    new_key = blended(ranks, 0, done, key, [got_key] * 2, [to_side(got_key)] * 2, done)
    got_value, new_key, small = lax.optimization_barrier((got_value, new_key, small))
    new_value = placed(ranks, new_value, got_value, to_side(got_value))
    return (new_query, new_key, new_value, *small)


def solution(mesh):
    in_specs = (
        P(("site", "rows"), "width"),
        P(("site", "rows"), "width"),
        P(("site", "rows"), "width"),
        P(("site", "rows"), "width"),
        P(("site", "rows"), "width"),
        P(("site", "rows"), "width"),
        P(("site", "rows")),
        P(("site", "rows", "width")),
        P(("site", "rows", "width")),
    )
    out_specs = (
        P("site", "width"),
        P("site", "width"),
        P("site", "width"),
        P(("site", "width")),
        P(("site", "width")),
        P(("site", "width")),
        P("site"),
    )
    body = functools.partial(shards, mesh.shape["rows"], mesh.shape["width"])

    return jax.shard_map(
        body, mesh=mesh, in_specs=in_specs, out_specs=out_specs, check_vma=False
    )
```

```python
import functools

import jax
import jax.numpy as jnp
from jax import lax
from jax.experimental import pallas as pl
from jax.experimental.pallas import tpu as pltpu
from jax.sharding import PartitionSpec as P


MESH = pl.DeviceIdType.MESH
CORES = 2
LANES = 128
LATE = 2
AHEAD = 3
HEAD = 160


def merge(
    ranks,
    widths,
    one_query,
    other_query,
    one_key,
    other_key,
    one_value,
    other_value,
    mix_share,
    norm_train,
    norm_step,
    query,
    key,
    value,
    far_early,
    far_query,
    far_key,
    far_value,
    far_rest,
    scale_query,
    scale_key,
    scale_value,
    all_norms,
    one,
    other,
    narrow,
    mix_row,
    mix,
    steps,
    norms,
    scales,
    peaks,
    head,
    narrow_head,
    small_sem,
    load_sem,
    out_sem,
    scale_sem,
    far_sem,
    peak_send,
    peak_recv,
    norm_send,
    norm_recv,
    wide_send,
    wide_recv,
    up_send,
    up_recv,
    down_send,
    down_recv,
    side_send,
    side_recv,
    early_send,
    early_recv,
    head_send,
    head_recv,
    head_out,
):
    depth, span = one_key.shape
    parts = one_query.shape[1] // span
    early = parts - LATE
    chips = ranks // CORES
    me = lax.axis_index("rows")
    across = lax.axis_index("width")
    chip, core = me // CORES, me % CORES
    partner = chip * CORES + 1 - core
    last = early - 1
    block = 32 if depth % 32 == 0 else depth
    late_parts = range(early, parts + 2)
    taken = head.shape[0]
    rest = pl.ds(taken, depth - taken)

    def is_static(k):
        return isinstance(k, int)

    def loads(k):
        if is_static(k) and k >= parts:
            sources = (one_key, other_key) if k == parts else (one_value, other_value)
        else:
            cut = pl.ds(pl.multiple_of(k * span, span), span)
            sources = one_query.at[:, cut], other_query.at[:, cut]
        return [
            pltpu.make_async_copy(source, target.at[k], load_sem.at[i, k])
            for i, (source, target) in enumerate(zip(sources, (one, other)))
        ]

    def load(k):
        for copy in loads(k):
            copy.start()

    barrier = pltpu.get_barrier_semaphore()

    @pl.loop(1, ranks)
    def _(step):
        to = {"rows": lax.rem(me + step, ranks)}
        pl.semaphore_signal(barrier, inc=1, device_id=to, device_id_type=MESH)

    @pl.loop(1, widths)
    def _(step):
        to = {"width": lax.rem(across + step, widths)}
        pl.semaphore_signal(barrier, inc=1, device_id=to, device_id_type=MESH)

    small = [
        pltpu.make_async_copy(mix_share, mix_row, small_sem.at[0]),
        pltpu.make_async_copy(norm_train, steps.at[0], small_sem.at[1]),
        pltpu.make_async_copy(norm_step, steps.at[1], small_sem.at[2]),
    ]
    for copy in small:
        copy.start()

    pl.loop(0, AHEAD)(load)

    for copy in small:
        copy.wait()
    norms[across, me] = steps[0] + steps[1]

    for i in range(mix_row.shape[0]):
        row = jnp.broadcast_to(mix_row[i : i + 1], (LANES, LANES))
        mix[i * LANES : (i + 1) * LANES] = row.T

    def send_peaks(k):
        @pl.loop(1, ranks)
        def _(step):
            pltpu.make_async_remote_copy(
                src_ref=peaks.at[k, me],
                dst_ref=peaks.at[k, me],
                send_sem=peak_send.at[k],
                recv_sem=peak_recv.at[k],
                device_id={"rows": lax.rem(me + step, ranks)},
                device_id_type=MESH,
            ).start()

    def mixed(k):
        for copy in loads(k):
            copy.wait()
        if is_static(k):
            if k + AHEAD < parts + 2:
                load(k + AHEAD)
        else:

            @pl.when(k + AHEAD < parts)
            def _():
                load(k + AHEAD)

            for tail in (parts, parts + 1):

                @pl.when(k + AHEAD == tail)
                def _():
                    load(tail)

        def step(b, top):
            rows = pl.ds(pl.multiple_of(b * block, block), block)
            share = jnp.concatenate([mix[rows]] * (span // LANES), axis=1)
            whole = share * one[k, rows] + (1.0 - share) * other[k, rows]
            one[k, rows] = whole
            return jnp.maximum(top, jnp.max(jnp.abs(whole).reshape(-1, 8, span), axis=0))

        top = lax.fori_loop(0, depth // block, step, jnp.zeros((8, span), jnp.float32))
        peaks[k, me] = jnp.max(top, axis=0, keepdims=True)

    def is_tail(k):
        return is_static(k) and k >= parts

    def hops(k):
        return chips - 2 if is_static(k) and k >= early else chips - 1

    def slot(k, rank):
        rows = pl.ds(pl.multiple_of(rank * depth, depth), depth)
        if is_tail(k):
            return (key if k == parts else value).at[rows]
        return query.at[rows, pl.ds(pl.multiple_of(k * span, span), span)]

    def send(k, rank, to, send_sem, recv_sem, source=None, cut=None):
        target = slot(k, rank)
        source = target if source is None else source
        if cut is not None:
            source, target = source.at[cut], target.at[cut]
        return pltpu.make_async_remote_copy(
            src_ref=source,
            dst_ref=target,
            send_sem=send_sem,
            recv_sem=recv_sem,
            device_id={"rows": to},
            device_id_type=MESH,
        )

    def go_up(k, hop, source=None, cut=None):
        sems = up_send.at[hop, k], up_recv.at[hop, k]
        return send(k, me - CORES * hop, me + CORES, *sems, source, cut)

    def go_down(k, hop, source=None, cut=None):
        sems = down_send.at[hop, k], down_recv.at[hop, k]
        return send(k, me + CORES * hop, me - CORES, *sems, source, cut)

    def go_side(k, hop, source=None, cut=None):
        index = hop + chips - 1
        sems = side_send.at[index, k], side_recv.at[index, k]
        return send(k, me + CORES * hop, partner, *sems, source, cut)

    def from_side(k, hop):
        index = hop + chips - 1
        return send(
            k, partner + CORES * hop, partner, side_send.at[index, k], side_recv.at[index, k]
        )

    def from_below(k, hop, cut=None):
        sems = up_send.at[hop, k], up_recv.at[hop, k]
        return send(k, me - CORES * (hop + 1), me - CORES, *sems, None, cut)

    def from_above(k, hop, cut=None):
        sems = down_send.at[hop, k], down_recv.at[hop, k]
        return send(k, me + CORES * (hop + 1), me + CORES, *sems, None, cut)

    def whole_or_rest(k, headed, action):
        if is_static(k):
            action(None)
            return
        headed = headed & (k == 0)
        pl.when(headed)(lambda: action(rest))
        pl.when(jnp.logical_not(headed))(lambda: action(None))

    has_below, has_above = chip >= 1, chip < chips - 1

    def keep(k):
        return pltpu.make_async_copy(narrow.at[k], slot(k, me), out_sem.at[k])

    def keep_scale(k):
        if is_tail(k):
            target = scale_key if k == parts else scale_value
        else:
            target = scale_query.at[:, pl.ds(pl.multiple_of(k * span, span), span)]
        return pltpu.make_async_copy(scales.at[k], target, scale_sem.at[k])

    def scaled(k):
        everyone = peaks.at[k, pl.ds(0, ranks - 1)]
        pltpu.make_async_copy(everyone, everyone, peak_recv.at[k]).wait()
        scale = jnp.max(peaks[k], axis=0)
        scales[k] = scale

        @pl.loop(0, depth // block)
        def _(b):
            rows = pl.ds(pl.multiple_of(b * block, block), block)
            narrow[k, rows] = (one[k, rows] / scale).astype(jnp.bfloat16)

        source = narrow.at[k]

        @pl.when(has_below)
        def _():
            whole_or_rest(k, chip == 1, lambda cut: go_down(k, 0, source, cut).start())

        @pl.when(has_above)
        def _():
            whole_or_rest(k, chip == chips - 2, lambda cut: go_up(k, 0, source, cut).start())

        go_side(k, 0, source).start()
        keep(k).start()
        keep_scale(k).start()

    lag = min(3, parts)
    pl.loop(0, lag)(mixed)
    pl.semaphore_wait(barrier, ranks + widths - 2)
    pl.loop(0, lag)(send_peaks)

    def send_head(to):
        return pltpu.make_async_remote_copy(
            src_ref=one.at[0, pl.ds(0, taken)],
            dst_ref=head,
            send_sem=head_send,
            recv_sem=head_recv,
            device_id={"rows": to},
            device_id_type=MESH,
        )

    near_end = (chip == 1) | (chip == chips - 2)
    at_end = (chip == 0) | (chip == chips - 1)
    near_rank = jnp.where(chip == 0, me + CORES, me - CORES)

    @pl.when(near_end)
    def _():
        send_head(jnp.where(chip == 1, me - CORES, me + CORES)).start()

    def advance(k):
        mixed(k)
        send_peaks(k)

    ahead = min(lag + 1, parts)
    pl.loop(lag, ahead)(advance)

    def head_slot():
        return slot(jnp.int32(0), near_rank).at[pl.ds(0, taken)]

    def keep_head():
        return pltpu.make_async_copy(narrow_head, head_slot(), head_out)

    @pl.loop(0, parts - ahead)
    def _(k):
        scaled(k)
        advance(k + ahead)

        @pl.when(at_end & (k == 0))
        def _():
            send_head(near_rank).wait_recv()
            narrow_head[...] = (head[...] / scales[0]).astype(jnp.bfloat16)
            keep_head().start()
            hop = jnp.where(chip == 0, 1, -1)
            index = hop + chips - 1
            pltpu.make_async_remote_copy(
                src_ref=narrow_head,
                dst_ref=head_slot(),
                send_sem=side_send.at[index, 0],
                recv_sem=side_recv.at[index, 0],
                device_id={"rows": partner},
                device_id_type=MESH,
            ).start()

    advance(parts)
    advance(parts + 1)

    @pl.loop(1, ranks)
    def _(step):
        pltpu.make_async_remote_copy(
            src_ref=norms.at[across, me],
            dst_ref=norms.at[across, me],
            send_sem=norm_send,
            recv_sem=norm_recv,
            device_id={"rows": lax.rem(me + step, ranks)},
            device_id_type=MESH,
        ).start()

    pl.loop(parts - ahead, parts)(scaled)
    scaled(parts)
    scaled(parts + 1)

    others = norms.at[across, pl.ds(0, ranks - 1)]
    pltpu.make_async_copy(others, others, norm_recv).wait()

    @pl.loop(1, widths)
    def _(step):
        pltpu.make_async_remote_copy(
            src_ref=norms.at[across],
            dst_ref=norms.at[across],
            send_sem=wide_send,
            recv_sem=wide_recv,
            device_id={"width": lax.rem(across + step, widths)},
            device_id_type=MESH,
        ).start()

    def far_copies(k, rank):
        source, at = slot(k, rank), far_sem.at[k - last]
        if k <= parts:
            if k == last:
                target = far_early
            elif k == parts:
                target = far_key
            else:
                target = far_query.at[:, pl.ds((k - early) * span, span)]
            return [pltpu.make_async_copy(source, target, at)]
        most = far_value.shape[0]
        return [
            pltpu.make_async_copy(source.at[pl.ds(0, most)], far_value, at),
            pltpu.make_async_copy(
                source.at[pl.ds(most, depth - most)], far_rest, far_sem.at[k - last + 1]
            ),
        ]

    def last_early(rank, to):
        return pltpu.make_async_remote_copy(
            src_ref=slot(last, rank),
            dst_ref=far_early,
            send_sem=early_send,
            recv_sem=early_recv,
            device_id={"rows": to},
            device_id_type=MESH,
        )

    def relay(k, hop):
        is_far = is_static(k)
        is_last = is_static(k) and k == last
        onward = hop < (chips - 2 if is_last else hops(k))

        @pl.when(chip >= hop)
        def _():
            headed = (chip == chips - 1) & (hop == 1)
            whole_or_rest(k, headed, lambda cut: from_below(k, hop - 1, cut).wait_recv())

            @pl.when(has_above & onward)
            def _():
                go_up(k, hop).start()

            whole_or_rest(k, headed, lambda cut: go_side(k, -hop, None, cut).start())

            if is_last:

                @pl.when((hop == chips - 2) & has_above & (core == 1))
                def _():
                    last_early(me - CORES * hop, me + CORES).start()

            if is_far:

                @pl.when((hop == chips - 2) & (chip == chips - 2))
                def _():
                    for copy in far_copies(k, me - CORES * hop):
                        copy.start()

        @pl.when(chip + hop < chips)
        def _():
            headed = (chip == 0) & (hop == 1)
            whole_or_rest(k, headed, lambda cut: from_above(k, hop - 1, cut).wait_recv())

            @pl.when(has_below & onward)
            def _():
                go_down(k, hop).start()

            whole_or_rest(k, headed, lambda cut: go_side(k, hop, None, cut).start())

            if is_last:

                @pl.when((hop == chips - 2) & has_below & (core == 1))
                def _():
                    last_early(me + CORES * hop, me - CORES).start()

            if is_far:

                @pl.when((hop == chips - 2) & (chip == 1))
                def _():
                    for copy in far_copies(k, me + CORES * hop):
                        copy.start()

    @pl.loop(1, chips - 1)
    def _(hop):
        pl.loop(0, last)(lambda k: relay(k, hop))
        relay(last, hop)
        for k in late_parts:
            relay(k, hop)

    def finish(k):
        keep(k).wait()
        keep_scale(k).wait()
        most = chips - 2 if is_static(k) else chips - 1

        @pl.loop(0, most)
        def _(hop):
            @pl.when((chip >= hop) & has_above)
            def _():
                headed = (chip == chips - 2) & (hop == 0)
                whole_or_rest(k, headed, lambda cut: go_up(k, hop, None, cut).wait_send())

            @pl.when((chip + hop < chips) & has_below)
            def _():
                headed = (chip == 1) & (hop == 0)
                whole_or_rest(k, headed, lambda cut: go_down(k, hop, None, cut).wait_send())

        @pl.loop(0, chips)
        def _(origin):
            @pl.when((origin - chip <= most) & (chip - origin <= most))
            def _():
                go_side(k, origin - chip).wait_send()
                from_side(k, origin - chip).wait_recv()

    def settle(k):
        everyone = peaks.at[k, pl.ds(0, ranks - 1)]
        pltpu.make_async_copy(everyone, everyone, peak_send.at[k]).wait()

    for k in (last, *late_parts):
        finish(k)

        @pl.when(near_end)
        def _():
            for copy in far_copies(k, me):
                copy.wait()

    @pl.when(near_end)
    def _():
        send_head(partner).wait_send()

    @pl.when(at_end)
    def _():
        keep_head().wait()

    pl.loop(0, parts + 2)(settle)
    pltpu.make_async_copy(others, others, norm_send).wait()
    around = norms.at[pl.ds(0, widths - 1)]
    pltpu.make_async_copy(around, around, wide_recv).wait()
    pltpu.make_async_copy(around, around, wide_send).wait()
    keep_norms = pltpu.make_async_copy(norms, all_norms, small_sem.at[3])
    keep_norms.start()
    keep_norms.wait()

    @pl.loop(0, last)
    def _(k):
        relay(k, chips - 1)

        @pl.when(k > 0)
        def _():
            finish(k - 1)

    if last > 0:
        finish(jnp.int32(last - 1))

    @pl.when(at_end & (core == 1))
    def _():
        last_early(me, partner).wait_recv()

    @pl.when(near_end & (core == 1))
    def _():
        last_early(me, partner).wait_send()


def stream(total, incoming, outgoing, ring):
    ahead = ring // 2

    def head():
        for i in range(min(ahead, total)):
            incoming(i, True)

    def body():
        @pl.loop(0, total)
        def _(i):
            incoming(i, False)
            outgoing(i).start()

            @pl.when(i + ahead < total)
            def _():
                @pl.when(i + ahead >= ring)
                def _():
                    outgoing(i + ahead - ring).wait()

                incoming(i + ahead, True)

    def drain():
        @pl.loop(max(0, total - ring), total)
        def _(i):
            outgoing(i).wait()

    return head, body, drain


def act(copy, begin):
    if begin:
        copy.start()
    else:
        copy.wait()


def settle_kernel(
    query,
    value,
    scale_key,
    scale_value,
    new_query,
    new_value,
    new_scale_key,
    new_scale_value,
    done,
    wide_buf,
    slim_buf,
    sems,
):
    ring = wide_buf.shape[0]

    def plan(source, target, buf, at):
        step = buf.shape[1]
        cols = pl.ds(0, buf.shape[2])

        def rows(i):
            return pl.ds(pl.multiple_of(i * step, step), step)

        def incoming(i, begin):
            place = lax.rem(i, ring)
            act(
                pltpu.make_async_copy(
                    source.at[rows(i), cols], buf.at[place], sems.at[at, place]
                ),
                begin,
            )

        def outgoing(i):
            place = lax.rem(i, ring)
            return pltpu.make_async_copy(
                buf.at[place], target.at[rows(i), cols], sems.at[at + 1, place]
            )

        return stream(source.shape[0] // step, incoming, outgoing, ring)

    first = plan(query, new_query, wide_buf, 0)
    second = plan(value, new_value, slim_buf, 2)
    first[0]()
    first[1]()
    second[0]()
    second[1]()
    first[2]()
    second[2]()
    new_scale_key[...] = scale_key[...]
    new_scale_value[...] = scale_value[...]
    done[...] = jnp.zeros_like(done)


def chunk_of(rows, most):
    step = rows
    while step > most and step % 32 == 0:
        step //= 2
    return step


def settled(query, value, scale_key, scale_value, wide, ring=8):
    rows, span = value.shape
    step = chunk_of(rows, 256)
    slim = chunk_of(rows, 512)
    anywhere = pl.BlockSpec(memory_space=pl.ANY)
    near = pl.BlockSpec(memory_space=pltpu.VMEM)
    moved = 4 * rows * (wide + span)
    return pl.pallas_call(
        settle_kernel,
        out_shape=(
            jax.ShapeDtypeStruct(query.shape, query.dtype),
            jax.ShapeDtypeStruct(value.shape, value.dtype),
            jax.ShapeDtypeStruct(scale_key.shape, scale_key.dtype),
            jax.ShapeDtypeStruct(scale_value.shape, scale_value.dtype),
            jax.ShapeDtypeStruct((8, LANES), jnp.float32),
        ),
        in_specs=[anywhere, anywhere, near, near],
        out_specs=(anywhere, anywhere, near, near, near),
        scratch_shapes=[
            pltpu.VMEM((ring, step, wide), query.dtype),
            pltpu.VMEM((ring, slim, span), value.dtype),
            pltpu.SemaphoreType.DMA((4, ring)),
        ],
        compiler_params=pltpu.CompilerParams(vmem_limit_bytes=60 * 2**20),
        cost_estimate=pl.CostEstimate(
            flops=0, bytes_accessed=moved, transcendentals=0
        ),
    )(query, value, scale_key, scale_value)


def far_ranks(ranks):
    chips = ranks // CORES
    me = lax.axis_index("rows")
    chip, core = me // CORES, me % CORES
    at_end = (chip == 0) | (chip == chips - 1)
    away = jnp.where(chip == 0, chips - 1, 0) * CORES
    return at_end, away + core, away + 1 - core


def blend_kernel(ranks, first, fresh, whole, got0, got1, side0, side1, done, target, buf, sems):
    at_end, straight, crossed = far_ranks(ranks)
    core = lax.axis_index("rows") % CORES
    ring, depth, span = buf.shape
    cols = pl.ds(first, span)

    def rows(i):
        return pl.ds(pl.multiple_of(i * depth, depth), depth)

    def incoming(i, begin):
        place = lax.rem(i, ring)

        def copy(origin):
            act(pltpu.make_async_copy(origin, buf.at[place], sems.at[0, place]), begin)

        if not begin:
            copy(whole.at[rows(i), cols])
            return
        is_got = at_end & (i == straight)
        is_side = at_end & (i == crossed)
        pl.when(is_got & (core == 0))(lambda: copy(got0))
        pl.when(is_got & (core == 1))(lambda: copy(got1))
        pl.when(is_side & (core == 0))(lambda: copy(side0))
        pl.when(is_side & (core == 1))(lambda: copy(side1))
        pl.when(jnp.logical_not(is_got | is_side))(lambda: copy(whole.at[rows(i), cols]))

    def outgoing(i):
        place = lax.rem(i, ring)
        return pltpu.make_async_copy(
            buf.at[place], target.at[rows(i), cols], sems.at[1, place]
        )

    for phase in stream(ranks, incoming, outgoing, ring):
        phase()


def blended(ranks, first, fresh, whole, gots, sides, done, ring=6):
    anywhere = pl.BlockSpec(memory_space=pl.ANY)
    return pl.pallas_call(
        functools.partial(blend_kernel, ranks, first),
        out_shape=jax.ShapeDtypeStruct(whole.shape, whole.dtype),
        in_specs=[anywhere] * 7,
        out_specs=anywhere,
        scratch_shapes=[
            pltpu.VMEM((ring, *gots[0].shape), whole.dtype),
            pltpu.SemaphoreType.DMA((2, ring)),
        ],
        input_output_aliases={} if fresh is done else {0: 0},
        compiler_params=pltpu.CompilerParams(vmem_limit_bytes=60 * 2**20),
        cost_estimate=pl.CostEstimate(
            flops=0, bytes_accessed=4 * ranks * gots[0].size, transcendentals=0
        ),
    )(fresh, whole, *gots, *sides, done)


def place_kernel(ranks, depth, _, *refs):
    gots, sides, (target, sems) = refs[0:2], refs[2:4], refs[4:]
    at_end, straight, crossed = far_ranks(ranks)

    @pl.when(at_end)
    def _():
        copies = []
        for rank, pieces in ((straight, gots), (crossed, sides)):
            row = rank * depth
            for piece in pieces:
                rows = pl.ds(pl.multiple_of(row, 8), piece.shape[0])
                at = sems.at[len(copies)]
                copies.append(pltpu.make_async_copy(piece, target.at[rows], at))
                row = row + piece.shape[0]
        for copy in copies:
            copy.start()
        for copy in copies:
            copy.wait()


def placed(ranks, whole, gots, sides):
    anywhere = pl.BlockSpec(memory_space=pl.ANY)
    near = pl.BlockSpec(memory_space=pltpu.VMEM)
    depth = whole.shape[0] // ranks
    return pl.pallas_call(
        functools.partial(place_kernel, ranks, depth),
        out_shape=jax.ShapeDtypeStruct(whole.shape, whole.dtype),
        in_specs=[anywhere, near, near, near, near],
        out_specs=anywhere,
        scratch_shapes=[pltpu.SemaphoreType.DMA((4,))],
        input_output_aliases={0: 0},
        compiler_params=pltpu.CompilerParams(vmem_limit_bytes=8 * 2**20),
        cost_estimate=pl.CostEstimate(
            flops=0, bytes_accessed=8 * gots[0].size, transcendentals=0
        ),
    )(whole, *gots, *sides)


def shards(
    ranks,
    widths,
    one_query,
    other_query,
    one_key,
    other_key,
    one_value,
    other_value,
    mix_share,
    norm_train,
    norm_step,
):
    depth, span = one_key.shape
    wide = one_query.shape[1]
    parts = wide // span
    chips = ranks // CORES
    bit = norm_train.shape[0]
    late = LATE * span
    tail = max(8, depth // 64 * 8)
    head = min(HEAD, depth // 16 * 8)
    tall = -(-depth // LANES) * LANES
    if tall != depth:
        mix_share = jnp.pad(mix_share, (0, tall - depth))
    mix_rows = mix_share.reshape(tall // LANES, LANES)
    shape = jax.ShapeDtypeStruct
    anywhere = pl.BlockSpec(memory_space=pl.ANY)
    dma = pltpu.SemaphoreType.DMA
    (
        query, key, value, far_early, far_query, far_key, far_value, far_rest,
        scale_query, scale_key, scale_value, norms,
    ) = pl.pallas_call(
        functools.partial(merge, ranks, widths),
        out_shape=(
            shape((ranks * depth, wide), jnp.bfloat16),
            shape((ranks * depth, span), jnp.bfloat16),
            shape((ranks * depth, span), jnp.bfloat16),
            shape((depth, span), jnp.bfloat16),
            shape((depth, late), jnp.bfloat16),
            shape((depth, span), jnp.bfloat16),
            shape((depth - tail, span), jnp.bfloat16),
            shape((tail, span), jnp.bfloat16),
            shape((1, wide), jnp.float32),
            shape((1, span), jnp.float32),
            shape((1, span), jnp.float32),
            shape((widths, ranks, 1, bit), jnp.float32),
        ),
        in_specs=[anywhere] * 9,
        out_specs=[anywhere] * 12,
        scratch_shapes=[
            pltpu.VMEM((parts + 2, depth, span), jnp.float32),
            pltpu.VMEM((parts + 2, depth, span), jnp.float32),
            pltpu.VMEM((parts + 2, depth, span), jnp.bfloat16),
            pltpu.VMEM(mix_rows.shape, jnp.float32),
            pltpu.VMEM((tall, LANES), jnp.float32),
            pltpu.VMEM((2, 1, bit), jnp.float32),
            pltpu.VMEM((widths, ranks, 1, bit), jnp.float32),
            pltpu.VMEM((parts + 2, 1, span), jnp.float32),
            pltpu.VMEM((parts + 2, ranks, 1, span), jnp.float32),
            pltpu.VMEM((head, span), jnp.float32),
            pltpu.VMEM((head, span), jnp.bfloat16),
            dma((4,)),
            dma((2, parts + 2)),
            dma((parts + 2,)),
            dma((parts + 2,)),
            dma((LATE + 4,)),
            dma((parts + 2,)),
            dma((parts + 2,)),
            dma,
            dma,
            dma,
            dma,
            dma((chips - 1, parts + 2)),
            dma((chips - 1, parts + 2)),
            dma((chips - 1, parts + 2)),
            dma((chips - 1, parts + 2)),
            dma((2 * chips - 1, parts + 2)),
            dma((2 * chips - 1, parts + 2)),
            dma,
            dma,
            dma,
            dma,
            dma,
        ],
        compiler_params=pltpu.CompilerParams(
            collective_id=0, has_side_effects=True, vmem_limit_bytes=56 * 2**20
        ),
    )(
        one_query,
        other_query,
        one_key,
        other_key,
        one_value,
        other_value,
        mix_rows,
        norm_train[None],
        norm_step[None],
    )
    first = wide - late - span
    ends = ((1, 0), (chips - 2, chips - 1))

    def send(piece, *pairs):
        return lax.ppermute(
            piece,
            "rows",
            [
                (source * CORES + a, target * CORES + b)
                for near, end in ends
                for hop in pairs
                for (source, a), (target, b) in [
                    ((near if hop[0] else end, hop[1]), (end, hop[2]))
                ]
            ],
        )

    def last_hop(piece):
        return send(piece, (True, 0, 0), (True, 1, 1))

    def to_side(piece):
        return send(piece, (False, 0, 1), (False, 1, 0))

    got_early = send(far_early, (True, 0, 0))
    got_query = last_hop(far_query)
    got_key = last_hop(far_key)
    got_value = last_hop(far_value)
    got_rest = last_hop(far_rest)
    new_query, new_value, scale_key, scale_value, done = settled(
        query, value, scale_key, scale_value, first
    )
    small = (
        scale_query[0],
        scale_key[0],
        scale_value[0],
        norms.transpose(1, 0, 2, 3).reshape(-1).astype(jnp.bfloat16),
    )
    got_early, far_early, done = lax.optimization_barrier((got_early, far_early, done))
    sides = send(far_early, (False, 1, 0)), send(got_early, (False, 0, 1))
    new_query = blended(
        ranks, first, new_query, query, (got_early, far_early), sides, done
    )
    got_query, new_query = lax.optimization_barrier((got_query, new_query))
    new_query = blended(
        ranks, first + span, new_query, query, [got_query] * 2, [to_side(got_query)] * 2, done
    )
    got_key, new_query = lax.optimization_barrier((got_key, new_query))
    new_key = blended(ranks, 0, done, key, [got_key] * 2, [to_side(got_key)] * 2, done)
    got_value, new_key, small = lax.optimization_barrier((got_value, new_key, small))
    sides = to_side(got_value), to_side(got_rest)
    new_value = placed(ranks, new_value, (got_value, got_rest), sides)
    return (new_query, new_key, new_value, *small)


def solution(mesh):
    in_specs = (
        P(("site", "rows"), "width"),
        P(("site", "rows"), "width"),
        P(("site", "rows"), "width"),
        P(("site", "rows"), "width"),
        P(("site", "rows"), "width"),
        P(("site", "rows"), "width"),
        P(("site", "rows")),
        P(("site", "rows", "width")),
        P(("site", "rows", "width")),
    )
    out_specs = (
        P("site", "width"),
        P("site", "width"),
        P("site", "width"),
        P(("site", "width")),
        P(("site", "width")),
        P(("site", "width")),
        P("site"),
    )
    body = functools.partial(shards, mesh.shape["rows"], mesh.shape["width"])

    return jax.shard_map(
        body, mesh=mesh, in_specs=in_specs, out_specs=out_specs, check_vma=False
    )
```

```python
import functools

import jax
import jax.numpy as jnp
from jax import lax
from jax.experimental import pallas as pl
from jax.experimental.pallas import tpu as pltpu
from jax.sharding import PartitionSpec as P


MESH = pl.DeviceIdType.MESH
CORES = 2
LANES = 128
LATE = 2
AHEAD = 3
HEAD = 96


def merge(
    ranks,
    widths,
    one_query,
    other_query,
    one_key,
    other_key,
    one_value,
    other_value,
    mix_share,
    norm_train,
    norm_step,
    query,
    key,
    value,
    far_early,
    far_query,
    far_key,
    far_value,
    far_rest,
    scale_query,
    scale_key,
    scale_value,
    all_norms,
    one,
    other,
    narrow,
    mix_row,
    mix,
    steps,
    norms,
    scales,
    peaks,
    head,
    narrow_head,
    small_sem,
    load_sem,
    out_sem,
    scale_sem,
    far_sem,
    peak_send,
    peak_recv,
    norm_send,
    norm_recv,
    wide_send,
    wide_recv,
    up_send,
    up_recv,
    down_send,
    down_recv,
    side_send,
    side_recv,
    early_send,
    early_recv,
    head_send,
    head_recv,
    head_out,
):
    depth, span = one_key.shape
    parts = one_query.shape[1] // span
    early = parts - LATE
    chips = ranks // CORES
    me = lax.axis_index("rows")
    across = lax.axis_index("width")
    chip, core = me // CORES, me % CORES
    partner = chip * CORES + 1 - core
    last = early - 1
    block = 32 if depth % 32 == 0 else depth
    late_parts = range(early, parts + 2)
    taken = head.shape[0]
    rest = pl.ds(taken, depth - taken)

    def is_static(k):
        return isinstance(k, int)

    def loads(k):
        if is_static(k) and k >= parts:
            sources = (one_key, other_key) if k == parts else (one_value, other_value)
        else:
            cut = pl.ds(pl.multiple_of(k * span, span), span)
            sources = one_query.at[:, cut], other_query.at[:, cut]
        return [
            pltpu.make_async_copy(source, target.at[k], load_sem.at[i, k])
            for i, (source, target) in enumerate(zip(sources, (one, other)))
        ]

    def load(k):
        for copy in loads(k):
            copy.start()

    barrier = pltpu.get_barrier_semaphore()

    @pl.loop(1, ranks)
    def _(step):
        to = {"rows": lax.rem(me + step, ranks)}
        pl.semaphore_signal(barrier, inc=1, device_id=to, device_id_type=MESH)

    @pl.loop(1, widths)
    def _(step):
        to = {"width": lax.rem(across + step, widths)}
        pl.semaphore_signal(barrier, inc=1, device_id=to, device_id_type=MESH)

    small = [
        pltpu.make_async_copy(mix_share, mix_row, small_sem.at[0]),
        pltpu.make_async_copy(norm_train, steps.at[0], small_sem.at[1]),
        pltpu.make_async_copy(norm_step, steps.at[1], small_sem.at[2]),
    ]
    for copy in small:
        copy.start()

    pl.loop(0, AHEAD)(load)

    for copy in small:
        copy.wait()
    norms[across, me] = steps[0] + steps[1]

    for i in range(mix_row.shape[0]):
        row = jnp.broadcast_to(mix_row[i : i + 1], (LANES, LANES))
        mix[i * LANES : (i + 1) * LANES] = row.T

    def send_peaks(k):
        @pl.loop(1, ranks)
        def _(step):
            pltpu.make_async_remote_copy(
                src_ref=peaks.at[k, me],
                dst_ref=peaks.at[k, me],
                send_sem=peak_send.at[k],
                recv_sem=peak_recv.at[k],
                device_id={"rows": lax.rem(me + step, ranks)},
                device_id_type=MESH,
            ).start()

    def mixed(k):
        for copy in loads(k):
            copy.wait()
        if is_static(k):
            if k + AHEAD < parts + 2:
                load(k + AHEAD)
        else:

            @pl.when(k + AHEAD < parts)
            def _():
                load(k + AHEAD)

            for tail in (parts, parts + 1):

                @pl.when(k + AHEAD == tail)
                def _():
                    load(tail)

        def step(b, top):
            rows = pl.ds(pl.multiple_of(b * block, block), block)
            share = jnp.concatenate([mix[rows]] * (span // LANES), axis=1)
            whole = share * one[k, rows] + (1.0 - share) * other[k, rows]
            one[k, rows] = whole
            return jnp.maximum(top, jnp.max(jnp.abs(whole).reshape(-1, 8, span), axis=0))

        top = lax.fori_loop(0, depth // block, step, jnp.zeros((8, span), jnp.float32))
        peaks[k, me] = jnp.max(top, axis=0, keepdims=True)

    def is_tail(k):
        return is_static(k) and k >= parts

    def hops(k):
        return chips - 2 if is_static(k) and k >= early else chips - 1

    def slot(k, rank):
        rows = pl.ds(pl.multiple_of(rank * depth, depth), depth)
        if is_tail(k):
            return (key if k == parts else value).at[rows]
        return query.at[rows, pl.ds(pl.multiple_of(k * span, span), span)]

    def send(k, rank, to, send_sem, recv_sem, source=None, cut=None):
        target = slot(k, rank)
        source = target if source is None else source
        if cut is not None:
            source, target = source.at[cut], target.at[cut]
        return pltpu.make_async_remote_copy(
            src_ref=source,
            dst_ref=target,
            send_sem=send_sem,
            recv_sem=recv_sem,
            device_id={"rows": to},
            device_id_type=MESH,
        )

    def go_up(k, hop, source=None, cut=None):
        sems = up_send.at[hop, k], up_recv.at[hop, k]
        return send(k, me - CORES * hop, me + CORES, *sems, source, cut)

    def go_down(k, hop, source=None, cut=None):
        sems = down_send.at[hop, k], down_recv.at[hop, k]
        return send(k, me + CORES * hop, me - CORES, *sems, source, cut)

    def go_side(k, hop, source=None, cut=None):
        index = hop + chips - 1
        sems = side_send.at[index, k], side_recv.at[index, k]
        return send(k, me + CORES * hop, partner, *sems, source, cut)

    def from_side(k, hop):
        index = hop + chips - 1
        return send(
            k, partner + CORES * hop, partner, side_send.at[index, k], side_recv.at[index, k]
        )

    def from_below(k, hop, cut=None):
        sems = up_send.at[hop, k], up_recv.at[hop, k]
        return send(k, me - CORES * (hop + 1), me - CORES, *sems, None, cut)

    def from_above(k, hop, cut=None):
        sems = down_send.at[hop, k], down_recv.at[hop, k]
        return send(k, me + CORES * (hop + 1), me + CORES, *sems, None, cut)

    def whole_or_rest(k, headed, action):
        if is_static(k):
            action(None)
            return
        headed = headed & (k == 0)
        pl.when(headed)(lambda: action(rest))
        pl.when(jnp.logical_not(headed))(lambda: action(None))

    has_below, has_above = chip >= 1, chip < chips - 1

    def keep(k):
        return pltpu.make_async_copy(narrow.at[k], slot(k, me), out_sem.at[k])

    def keep_scale(k):
        if is_tail(k):
            target = scale_key if k == parts else scale_value
        else:
            target = scale_query.at[:, pl.ds(pl.multiple_of(k * span, span), span)]
        return pltpu.make_async_copy(scales.at[k], target, scale_sem.at[k])

    def scaled(k):
        everyone = peaks.at[k, pl.ds(0, ranks - 1)]
        pltpu.make_async_copy(everyone, everyone, peak_recv.at[k]).wait()
        scale = jnp.max(peaks[k], axis=0)
        scales[k] = scale

        @pl.loop(0, depth // block)
        def _(b):
            rows = pl.ds(pl.multiple_of(b * block, block), block)
            narrow[k, rows] = (one[k, rows] / scale).astype(jnp.bfloat16)

        source = narrow.at[k]

        @pl.when(has_below)
        def _():
            whole_or_rest(k, chip == 1, lambda cut: go_down(k, 0, source, cut).start())

        @pl.when(has_above)
        def _():
            whole_or_rest(k, chip == chips - 2, lambda cut: go_up(k, 0, source, cut).start())

        go_side(k, 0, source).start()
        keep(k).start()
        keep_scale(k).start()

    lag = min(3, parts)
    pl.loop(0, 1)(mixed)
    pl.semaphore_wait(barrier, ranks + widths - 2)
    pl.loop(0, 1)(send_peaks)

    def send_head(to):
        return pltpu.make_async_remote_copy(
            src_ref=one.at[0, pl.ds(0, taken)],
            dst_ref=head,
            send_sem=head_send,
            recv_sem=head_recv,
            device_id={"rows": to},
            device_id_type=MESH,
        )

    near_end = (chip == 1) | (chip == chips - 2)
    at_end = (chip == 0) | (chip == chips - 1)
    near_rank = jnp.where(chip == 0, me + CORES, me - CORES)

    @pl.when(near_end)
    def _():
        send_head(jnp.where(chip == 1, me - CORES, me + CORES)).start()

    def advance(k):
        mixed(k)
        send_peaks(k)

    pl.loop(1, lag)(advance)

    def head_slot():
        return slot(jnp.int32(0), near_rank).at[pl.ds(0, taken)]

    def keep_head():
        return pltpu.make_async_copy(narrow_head, head_slot(), head_out)

    @pl.loop(0, parts - lag)
    def _(k):
        scaled(k)
        advance(k + lag)

        @pl.when(at_end & (k == 0))
        def _():
            send_head(near_rank).wait_recv()
            narrow_head[...] = (head[...] / scales[0]).astype(jnp.bfloat16)
            keep_head().start()
            hop = jnp.where(chip == 0, 1, -1)
            index = hop + chips - 1
            pltpu.make_async_remote_copy(
                src_ref=narrow_head,
                dst_ref=head_slot(),
                send_sem=side_send.at[index, 0],
                recv_sem=side_recv.at[index, 0],
                device_id={"rows": partner},
                device_id_type=MESH,
            ).start()

    advance(parts)
    advance(parts + 1)

    @pl.loop(1, ranks)
    def _(step):
        pltpu.make_async_remote_copy(
            src_ref=norms.at[across, me],
            dst_ref=norms.at[across, me],
            send_sem=norm_send,
            recv_sem=norm_recv,
            device_id={"rows": lax.rem(me + step, ranks)},
            device_id_type=MESH,
        ).start()

    pl.loop(parts - lag, parts)(scaled)
    scaled(parts)
    scaled(parts + 1)

    others = norms.at[across, pl.ds(0, ranks - 1)]
    pltpu.make_async_copy(others, others, norm_recv).wait()

    @pl.loop(1, widths)
    def _(step):
        pltpu.make_async_remote_copy(
            src_ref=norms.at[across],
            dst_ref=norms.at[across],
            send_sem=wide_send,
            recv_sem=wide_recv,
            device_id={"width": lax.rem(across + step, widths)},
            device_id_type=MESH,
        ).start()

    def far_copies(k, rank):
        source, at = slot(k, rank), far_sem.at[k - last]
        if k <= parts:
            if k == last:
                target = far_early
            elif k == parts:
                target = far_key
            else:
                target = far_query.at[:, pl.ds((k - early) * span, span)]
            return [pltpu.make_async_copy(source, target, at)]
        most = far_value.shape[0]
        return [
            pltpu.make_async_copy(source.at[pl.ds(0, most)], far_value, at),
            pltpu.make_async_copy(
                source.at[pl.ds(most, depth - most)], far_rest, far_sem.at[k - last + 1]
            ),
        ]

    def last_early(rank, to):
        return pltpu.make_async_remote_copy(
            src_ref=slot(last, rank),
            dst_ref=far_early,
            send_sem=early_send,
            recv_sem=early_recv,
            device_id={"rows": to},
            device_id_type=MESH,
        )

    def relay(k, hop):
        is_far = is_static(k)
        is_last = is_static(k) and k == last
        onward = hop < (chips - 2 if is_last else hops(k))

        @pl.when(chip >= hop)
        def _():
            headed = (chip == chips - 1) & (hop == 1)
            whole_or_rest(k, headed, lambda cut: from_below(k, hop - 1, cut).wait_recv())

            @pl.when(has_above & onward)
            def _():
                go_up(k, hop).start()

            whole_or_rest(k, headed, lambda cut: go_side(k, -hop, None, cut).start())

            if is_last:

                @pl.when((hop == chips - 2) & has_above & (core == 1))
                def _():
                    last_early(me - CORES * hop, me + CORES).start()

            if is_far:

                @pl.when((hop == chips - 2) & (chip == chips - 2))
                def _():
                    for copy in far_copies(k, me - CORES * hop):
                        copy.start()

        @pl.when(chip + hop < chips)
        def _():
            headed = (chip == 0) & (hop == 1)
            whole_or_rest(k, headed, lambda cut: from_above(k, hop - 1, cut).wait_recv())

            @pl.when(has_below & onward)
            def _():
                go_down(k, hop).start()

            whole_or_rest(k, headed, lambda cut: go_side(k, hop, None, cut).start())

            if is_last:

                @pl.when((hop == chips - 2) & has_below & (core == 1))
                def _():
                    last_early(me + CORES * hop, me - CORES).start()

            if is_far:

                @pl.when((hop == chips - 2) & (chip == 1))
                def _():
                    for copy in far_copies(k, me + CORES * hop):
                        copy.start()

    @pl.loop(1, chips - 1)
    def _(hop):
        pl.loop(0, last)(lambda k: relay(k, hop))
        relay(last, hop)
        for k in late_parts:
            relay(k, hop)

    def finish(k):
        keep(k).wait()
        keep_scale(k).wait()
        most = chips - 2 if is_static(k) else chips - 1

        @pl.loop(0, most)
        def _(hop):
            @pl.when((chip >= hop) & has_above)
            def _():
                headed = (chip == chips - 2) & (hop == 0)
                whole_or_rest(k, headed, lambda cut: go_up(k, hop, None, cut).wait_send())

            @pl.when((chip + hop < chips) & has_below)
            def _():
                headed = (chip == 1) & (hop == 0)
                whole_or_rest(k, headed, lambda cut: go_down(k, hop, None, cut).wait_send())

        @pl.loop(0, chips)
        def _(origin):
            @pl.when((origin - chip <= most) & (chip - origin <= most))
            def _():
                go_side(k, origin - chip).wait_send()
                from_side(k, origin - chip).wait_recv()

    def settle(k):
        everyone = peaks.at[k, pl.ds(0, ranks - 1)]
        pltpu.make_async_copy(everyone, everyone, peak_send.at[k]).wait()

    for k in (last, *late_parts):
        finish(k)

        @pl.when(near_end)
        def _():
            for copy in far_copies(k, me):
                copy.wait()

    @pl.when(near_end)
    def _():
        send_head(partner).wait_send()

    @pl.when(at_end)
    def _():
        keep_head().wait()

    pl.loop(0, parts + 2)(settle)
    pltpu.make_async_copy(others, others, norm_send).wait()
    around = norms.at[pl.ds(0, widths - 1)]
    pltpu.make_async_copy(around, around, wide_recv).wait()
    pltpu.make_async_copy(around, around, wide_send).wait()
    keep_norms = pltpu.make_async_copy(norms, all_norms, small_sem.at[3])
    keep_norms.start()
    keep_norms.wait()

    @pl.loop(0, last)
    def _(k):
        relay(k, chips - 1)

        @pl.when(k > 0)
        def _():
            finish(k - 1)

    if last > 0:
        finish(jnp.int32(last - 1))

    @pl.when(at_end & (core == 1))
    def _():
        last_early(me, partner).wait_recv()

    @pl.when(near_end & (core == 1))
    def _():
        last_early(me, partner).wait_send()


def stream(total, incoming, outgoing, ring):
    ahead = ring // 2

    def head():
        for i in range(min(ahead, total)):
            incoming(i, True)

    def body():
        @pl.loop(0, total)
        def _(i):
            incoming(i, False)
            outgoing(i).start()

            @pl.when(i + ahead < total)
            def _():
                @pl.when(i + ahead >= ring)
                def _():
                    outgoing(i + ahead - ring).wait()

                incoming(i + ahead, True)

    def drain():
        @pl.loop(max(0, total - ring), total)
        def _(i):
            outgoing(i).wait()

    return head, body, drain


def act(copy, begin):
    if begin:
        copy.start()
    else:
        copy.wait()


def settle_kernel(
    query,
    value,
    scale_key,
    scale_value,
    new_query,
    new_value,
    new_scale_key,
    new_scale_value,
    done,
    wide_buf,
    slim_buf,
    sems,
):
    ring = wide_buf.shape[0]

    def plan(source, target, buf, at):
        step = buf.shape[1]
        cols = pl.ds(0, buf.shape[2])

        def rows(i):
            return pl.ds(pl.multiple_of(i * step, step), step)

        def incoming(i, begin):
            place = lax.rem(i, ring)
            act(
                pltpu.make_async_copy(
                    source.at[rows(i), cols], buf.at[place], sems.at[at, place]
                ),
                begin,
            )

        def outgoing(i):
            place = lax.rem(i, ring)
            return pltpu.make_async_copy(
                buf.at[place], target.at[rows(i), cols], sems.at[at + 1, place]
            )

        return stream(source.shape[0] // step, incoming, outgoing, ring)

    first = plan(query, new_query, wide_buf, 0)
    second = plan(value, new_value, slim_buf, 2)
    first[0]()
    first[1]()
    second[0]()
    second[1]()
    first[2]()
    second[2]()
    new_scale_key[...] = scale_key[...]
    new_scale_value[...] = scale_value[...]
    done[...] = jnp.zeros_like(done)


def chunk_of(rows, most):
    step = rows
    while step > most and step % 32 == 0:
        step //= 2
    return step


def settled(query, value, scale_key, scale_value, wide, ring=8):
    rows, span = value.shape
    step = chunk_of(rows, 256)
    slim = chunk_of(rows, 512)
    anywhere = pl.BlockSpec(memory_space=pl.ANY)
    near = pl.BlockSpec(memory_space=pltpu.VMEM)
    moved = 4 * rows * (wide + span)
    return pl.pallas_call(
        settle_kernel,
        out_shape=(
            jax.ShapeDtypeStruct(query.shape, query.dtype),
            jax.ShapeDtypeStruct(value.shape, value.dtype),
            jax.ShapeDtypeStruct(scale_key.shape, scale_key.dtype),
            jax.ShapeDtypeStruct(scale_value.shape, scale_value.dtype),
            jax.ShapeDtypeStruct((8, LANES), jnp.float32),
        ),
        in_specs=[anywhere, anywhere, near, near],
        out_specs=(anywhere, anywhere, near, near, near),
        scratch_shapes=[
            pltpu.VMEM((ring, step, wide), query.dtype),
            pltpu.VMEM((ring, slim, span), value.dtype),
            pltpu.SemaphoreType.DMA((4, ring)),
        ],
        compiler_params=pltpu.CompilerParams(vmem_limit_bytes=60 * 2**20),
        cost_estimate=pl.CostEstimate(
            flops=0, bytes_accessed=moved, transcendentals=0
        ),
    )(query, value, scale_key, scale_value)


def far_ranks(ranks):
    chips = ranks // CORES
    me = lax.axis_index("rows")
    chip, core = me // CORES, me % CORES
    at_end = (chip == 0) | (chip == chips - 1)
    away = jnp.where(chip == 0, chips - 1, 0) * CORES
    return at_end, away + core, away + 1 - core


def blend_kernel(ranks, first, fresh, whole, got0, got1, side0, side1, done, target, buf, sems):
    at_end, straight, crossed = far_ranks(ranks)
    core = lax.axis_index("rows") % CORES
    ring, depth, span = buf.shape
    cols = pl.ds(first, span)

    def rows(i):
        return pl.ds(pl.multiple_of(i * depth, depth), depth)

    def incoming(i, begin):
        place = lax.rem(i, ring)

        def copy(origin):
            act(pltpu.make_async_copy(origin, buf.at[place], sems.at[0, place]), begin)

        if not begin:
            copy(whole.at[rows(i), cols])
            return
        is_got = at_end & (i == straight)
        is_side = at_end & (i == crossed)
        pl.when(is_got & (core == 0))(lambda: copy(got0))
        pl.when(is_got & (core == 1))(lambda: copy(got1))
        pl.when(is_side & (core == 0))(lambda: copy(side0))
        pl.when(is_side & (core == 1))(lambda: copy(side1))
        pl.when(jnp.logical_not(is_got | is_side))(lambda: copy(whole.at[rows(i), cols]))

    def outgoing(i):
        place = lax.rem(i, ring)
        return pltpu.make_async_copy(
            buf.at[place], target.at[rows(i), cols], sems.at[1, place]
        )

    for phase in stream(ranks, incoming, outgoing, ring):
        phase()


def blended(ranks, first, fresh, whole, gots, sides, done, ring=6):
    anywhere = pl.BlockSpec(memory_space=pl.ANY)
    return pl.pallas_call(
        functools.partial(blend_kernel, ranks, first),
        out_shape=jax.ShapeDtypeStruct(whole.shape, whole.dtype),
        in_specs=[anywhere] * 7,
        out_specs=anywhere,
        scratch_shapes=[
            pltpu.VMEM((ring, *gots[0].shape), whole.dtype),
            pltpu.SemaphoreType.DMA((2, ring)),
        ],
        input_output_aliases={} if fresh is done else {0: 0},
        compiler_params=pltpu.CompilerParams(vmem_limit_bytes=60 * 2**20),
        cost_estimate=pl.CostEstimate(
            flops=0, bytes_accessed=4 * ranks * gots[0].size, transcendentals=0
        ),
    )(fresh, whole, *gots, *sides, done)


def place_kernel(ranks, depth, _, *refs):
    gots, sides, (target, sems) = refs[0:2], refs[2:4], refs[4:]
    at_end, straight, crossed = far_ranks(ranks)

    @pl.when(at_end)
    def _():
        copies = []
        for rank, pieces in ((straight, gots), (crossed, sides)):
            row = rank * depth
            for piece in pieces:
                rows = pl.ds(pl.multiple_of(row, 8), piece.shape[0])
                at = sems.at[len(copies)]
                copies.append(pltpu.make_async_copy(piece, target.at[rows], at))
                row = row + piece.shape[0]
        for copy in copies:
            copy.start()
        for copy in copies:
            copy.wait()


def placed(ranks, whole, gots, sides):
    anywhere = pl.BlockSpec(memory_space=pl.ANY)
    near = pl.BlockSpec(memory_space=pltpu.VMEM)
    depth = whole.shape[0] // ranks
    return pl.pallas_call(
        functools.partial(place_kernel, ranks, depth),
        out_shape=jax.ShapeDtypeStruct(whole.shape, whole.dtype),
        in_specs=[anywhere, near, near, near, near],
        out_specs=anywhere,
        scratch_shapes=[pltpu.SemaphoreType.DMA((4,))],
        input_output_aliases={0: 0},
        compiler_params=pltpu.CompilerParams(vmem_limit_bytes=8 * 2**20),
        cost_estimate=pl.CostEstimate(
            flops=0, bytes_accessed=8 * gots[0].size, transcendentals=0
        ),
    )(whole, *gots, *sides)


def shards(
    ranks,
    widths,
    one_query,
    other_query,
    one_key,
    other_key,
    one_value,
    other_value,
    mix_share,
    norm_train,
    norm_step,
):
    depth, span = one_key.shape
    wide = one_query.shape[1]
    parts = wide // span
    chips = ranks // CORES
    bit = norm_train.shape[0]
    late = LATE * span
    tail = max(8, depth // 64 * 8)
    head = min(HEAD, depth // 16 * 8)
    tall = -(-depth // LANES) * LANES
    if tall != depth:
        mix_share = jnp.pad(mix_share, (0, tall - depth))
    mix_rows = mix_share.reshape(tall // LANES, LANES)
    shape = jax.ShapeDtypeStruct
    anywhere = pl.BlockSpec(memory_space=pl.ANY)
    dma = pltpu.SemaphoreType.DMA
    (
        query, key, value, far_early, far_query, far_key, far_value, far_rest,
        scale_query, scale_key, scale_value, norms,
    ) = pl.pallas_call(
        functools.partial(merge, ranks, widths),
        out_shape=(
            shape((ranks * depth, wide), jnp.bfloat16),
            shape((ranks * depth, span), jnp.bfloat16),
            shape((ranks * depth, span), jnp.bfloat16),
            shape((depth, span), jnp.bfloat16),
            shape((depth, late), jnp.bfloat16),
            shape((depth, span), jnp.bfloat16),
            shape((depth - tail, span), jnp.bfloat16),
            shape((tail, span), jnp.bfloat16),
            shape((1, wide), jnp.float32),
            shape((1, span), jnp.float32),
            shape((1, span), jnp.float32),
            shape((widths, ranks, 1, bit), jnp.float32),
        ),
        in_specs=[anywhere] * 9,
        out_specs=[anywhere] * 12,
        scratch_shapes=[
            pltpu.VMEM((parts + 2, depth, span), jnp.float32),
            pltpu.VMEM((parts + 2, depth, span), jnp.float32),
            pltpu.VMEM((parts + 2, depth, span), jnp.bfloat16),
            pltpu.VMEM(mix_rows.shape, jnp.float32),
            pltpu.VMEM((tall, LANES), jnp.float32),
            pltpu.VMEM((2, 1, bit), jnp.float32),
            pltpu.VMEM((widths, ranks, 1, bit), jnp.float32),
            pltpu.VMEM((parts + 2, 1, span), jnp.float32),
            pltpu.VMEM((parts + 2, ranks, 1, span), jnp.float32),
            pltpu.VMEM((head, span), jnp.float32),
            pltpu.VMEM((head, span), jnp.bfloat16),
            dma((4,)),
            dma((2, parts + 2)),
            dma((parts + 2,)),
            dma((parts + 2,)),
            dma((LATE + 4,)),
            dma((parts + 2,)),
            dma((parts + 2,)),
            dma,
            dma,
            dma,
            dma,
            dma((chips - 1, parts + 2)),
            dma((chips - 1, parts + 2)),
            dma((chips - 1, parts + 2)),
            dma((chips - 1, parts + 2)),
            dma((2 * chips - 1, parts + 2)),
            dma((2 * chips - 1, parts + 2)),
            dma,
            dma,
            dma,
            dma,
            dma,
        ],
        compiler_params=pltpu.CompilerParams(
            collective_id=0, has_side_effects=True, vmem_limit_bytes=56 * 2**20
        ),
    )(
        one_query,
        other_query,
        one_key,
        other_key,
        one_value,
        other_value,
        mix_rows,
        norm_train[None],
        norm_step[None],
    )
    first = wide - late - span
    ends = ((1, 0), (chips - 2, chips - 1))

    def send(piece, *pairs):
        return lax.ppermute(
            piece,
            "rows",
            [
                (source * CORES + a, target * CORES + b)
                for near, end in ends
                for hop in pairs
                for (source, a), (target, b) in [
                    ((near if hop[0] else end, hop[1]), (end, hop[2]))
                ]
            ],
        )

    def last_hop(piece):
        return send(piece, (True, 0, 0), (True, 1, 1))

    def to_side(piece):
        return send(piece, (False, 0, 1), (False, 1, 0))

    got_early = send(far_early, (True, 0, 0))
    got_query = last_hop(far_query)
    got_key = last_hop(far_key)
    got_value = last_hop(far_value)
    got_rest = last_hop(far_rest)
    new_query, new_value, scale_key, scale_value, done = settled(
        query, value, scale_key, scale_value, first
    )
    small = (
        scale_query[0],
        scale_key[0],
        scale_value[0],
        norms.transpose(1, 0, 2, 3).reshape(-1).astype(jnp.bfloat16),
    )
    got_early, far_early, done = lax.optimization_barrier((got_early, far_early, done))
    sides = send(far_early, (False, 1, 0)), send(got_early, (False, 0, 1))
    new_query = blended(
        ranks, first, new_query, query, (got_early, far_early), sides, done
    )
    got_query, new_query = lax.optimization_barrier((got_query, new_query))
    new_query = blended(
        ranks, first + span, new_query, query, [got_query] * 2, [to_side(got_query)] * 2, done
    )
    got_key, new_query = lax.optimization_barrier((got_key, new_query))
    new_key = blended(ranks, 0, done, key, [got_key] * 2, [to_side(got_key)] * 2, done)
    got_value, new_key, small = lax.optimization_barrier((got_value, new_key, small))
    sides = to_side(got_value), to_side(got_rest)
    new_value = placed(ranks, new_value, (got_value, got_rest), sides)
    return (new_query, new_key, new_value, *small)


def solution(mesh):
    in_specs = (
        P(("site", "rows"), "width"),
        P(("site", "rows"), "width"),
        P(("site", "rows"), "width"),
        P(("site", "rows"), "width"),
        P(("site", "rows"), "width"),
        P(("site", "rows"), "width"),
        P(("site", "rows")),
        P(("site", "rows", "width")),
        P(("site", "rows", "width")),
    )
    out_specs = (
        P("site", "width"),
        P("site", "width"),
        P("site", "width"),
        P(("site", "width")),
        P(("site", "width")),
        P(("site", "width")),
        P("site"),
    )
    body = functools.partial(shards, mesh.shape["rows"], mesh.shape["width"])

    return jax.shard_map(
        body, mesh=mesh, in_specs=in_specs, out_specs=out_specs, check_vma=False
    )
```

```python
import functools

import jax
import jax.numpy as jnp
from jax import lax
from jax.experimental import pallas as pl
from jax.experimental.pallas import tpu as pltpu
from jax.sharding import PartitionSpec as P


MESH = pl.DeviceIdType.MESH
CORES = 2
LANES = 128
LATE = 2
AHEAD = 3
HEAD = 96


def merge(
    ranks,
    widths,
    one_query,
    other_query,
    one_key,
    other_key,
    one_value,
    other_value,
    mix_share,
    norm_train,
    norm_step,
    query,
    key,
    value,
    far_early,
    far_query,
    far_key,
    far_value,
    far_rest,
    scale_query,
    scale_key,
    scale_value,
    all_norms,
    one,
    other,
    narrow,
    mix_row,
    mix,
    steps,
    norms,
    scales,
    pairs,
    peaks,
    head,
    narrow_head,
    small_sem,
    load_sem,
    out_sem,
    scale_sem,
    far_sem,
    pair_send,
    pair_recv,
    peak_send,
    peak_recv,
    norm_send,
    norm_recv,
    wide_send,
    wide_recv,
    up_send,
    up_recv,
    down_send,
    down_recv,
    side_send,
    side_recv,
    early_send,
    early_recv,
    head_send,
    head_recv,
    head_out,
):
    depth, span = one_key.shape
    parts = one_query.shape[1] // span
    early = parts - LATE
    chips = ranks // CORES
    me = lax.axis_index("rows")
    across = lax.axis_index("width")
    chip, core = me // CORES, me % CORES
    partner = chip * CORES + 1 - core
    last = early - 1
    block = 32 if depth % 32 == 0 else depth
    late_parts = range(early, parts + 2)
    taken = head.shape[0]
    rest = pl.ds(taken, depth - taken)

    def is_static(k):
        return isinstance(k, int)

    def loads(k):
        if is_static(k) and k >= parts:
            sources = (one_key, other_key) if k == parts else (one_value, other_value)
        else:
            cut = pl.ds(pl.multiple_of(k * span, span), span)
            sources = one_query.at[:, cut], other_query.at[:, cut]
        return [
            pltpu.make_async_copy(source, target.at[k], load_sem.at[i, k])
            for i, (source, target) in enumerate(zip(sources, (one, other)))
        ]

    def load(k):
        for copy in loads(k):
            copy.start()

    barrier = pltpu.get_barrier_semaphore()

    @pl.loop(1, ranks)
    def _(step):
        to = {"rows": lax.rem(me + step, ranks)}
        pl.semaphore_signal(barrier, inc=1, device_id=to, device_id_type=MESH)

    @pl.loop(1, widths)
    def _(step):
        to = {"width": lax.rem(across + step, widths)}
        pl.semaphore_signal(barrier, inc=1, device_id=to, device_id_type=MESH)

    small = [
        pltpu.make_async_copy(mix_share, mix_row, small_sem.at[0]),
        pltpu.make_async_copy(norm_train, steps.at[0], small_sem.at[1]),
        pltpu.make_async_copy(norm_step, steps.at[1], small_sem.at[2]),
    ]
    for copy in small:
        copy.start()

    pl.loop(0, AHEAD)(load)

    for copy in small:
        copy.wait()
    norms[across, me] = steps[0] + steps[1]

    for i in range(mix_row.shape[0]):
        row = jnp.broadcast_to(mix_row[i : i + 1], (LANES, LANES))
        mix[i * LANES : (i + 1) * LANES] = row.T

    peaks[1:, chips:] = jnp.zeros((parts + 1, ranks - chips, 1, span), jnp.float32)

    def send_peaks(k, mine, stride):
        @pl.loop(1, ranks // stride)
        def _(step):
            pltpu.make_async_remote_copy(
                src_ref=peaks.at[k, mine],
                dst_ref=peaks.at[k, mine],
                send_sem=peak_send.at[k],
                recv_sem=peak_recv.at[k],
                device_id={"rows": lax.rem(me + stride * step, ranks)},
                device_id_type=MESH,
            ).start()

    def wait_peaks(k, sem):
        def wait(count):
            everyone = peaks.at[k, pl.ds(0, count)]
            pltpu.make_async_copy(everyone, everyone, sem.at[k]).wait()

        if is_static(k):
            wait(chips - 1 if k else ranks - 1)
            return
        pl.when(k == 0)(lambda: wait(ranks - 1))
        pl.when(k > 0)(lambda: wait(chips - 1))

    def pair(k):
        return pltpu.make_async_remote_copy(
            src_ref=pairs.at[k, core],
            dst_ref=pairs.at[k, core],
            send_sem=pair_send.at[k],
            recv_sem=pair_recv.at[k],
            device_id={"rows": partner},
            device_id_type=MESH,
        )

    def mixed(k):
        for copy in loads(k):
            copy.wait()
        if is_static(k):
            if k + AHEAD < parts + 2:
                load(k + AHEAD)
        else:

            @pl.when(k + AHEAD < parts)
            def _():
                load(k + AHEAD)

            for tail in (parts, parts + 1):

                @pl.when(k + AHEAD == tail)
                def _():
                    load(tail)

        def step(b, top):
            rows = pl.ds(pl.multiple_of(b * block, block), block)
            share = jnp.concatenate([mix[rows]] * (span // LANES), axis=1)
            whole = share * one[k, rows] + (1.0 - share) * other[k, rows]
            one[k, rows] = whole
            return jnp.maximum(top, jnp.max(jnp.abs(whole).reshape(-1, 8, span), axis=0))

        top = lax.fori_loop(0, depth // block, step, jnp.zeros((8, span), jnp.float32))
        return jnp.max(top, axis=0, keepdims=True)

    def is_tail(k):
        return is_static(k) and k >= parts

    def hops(k):
        return chips - 2 if is_static(k) and k >= early else chips - 1

    def slot(k, rank):
        rows = pl.ds(pl.multiple_of(rank * depth, depth), depth)
        if is_tail(k):
            return (key if k == parts else value).at[rows]
        return query.at[rows, pl.ds(pl.multiple_of(k * span, span), span)]

    def send(k, rank, to, send_sem, recv_sem, source=None, cut=None):
        target = slot(k, rank)
        source = target if source is None else source
        if cut is not None:
            source, target = source.at[cut], target.at[cut]
        return pltpu.make_async_remote_copy(
            src_ref=source,
            dst_ref=target,
            send_sem=send_sem,
            recv_sem=recv_sem,
            device_id={"rows": to},
            device_id_type=MESH,
        )

    def go_up(k, hop, source=None, cut=None):
        sems = up_send.at[hop, k], up_recv.at[hop, k]
        return send(k, me - CORES * hop, me + CORES, *sems, source, cut)

    def go_down(k, hop, source=None, cut=None):
        sems = down_send.at[hop, k], down_recv.at[hop, k]
        return send(k, me + CORES * hop, me - CORES, *sems, source, cut)

    def go_side(k, hop, source=None, cut=None):
        index = hop + chips - 1
        sems = side_send.at[index, k], side_recv.at[index, k]
        return send(k, me + CORES * hop, partner, *sems, source, cut)

    def from_side(k, hop):
        index = hop + chips - 1
        return send(
            k, partner + CORES * hop, partner, side_send.at[index, k], side_recv.at[index, k]
        )

    def from_below(k, hop, cut=None):
        sems = up_send.at[hop, k], up_recv.at[hop, k]
        return send(k, me - CORES * (hop + 1), me - CORES, *sems, None, cut)

    def from_above(k, hop, cut=None):
        sems = down_send.at[hop, k], down_recv.at[hop, k]
        return send(k, me + CORES * (hop + 1), me + CORES, *sems, None, cut)

    def whole_or_rest(k, headed, action):
        if is_static(k):
            action(None)
            return
        headed = headed & (k == 0)
        pl.when(headed)(lambda: action(rest))
        pl.when(jnp.logical_not(headed))(lambda: action(None))

    has_below, has_above = chip >= 1, chip < chips - 1

    def keep(k):
        return pltpu.make_async_copy(narrow.at[k], slot(k, me), out_sem.at[k])

    def keep_scale(k):
        if is_tail(k):
            target = scale_key if k == parts else scale_value
        else:
            target = scale_query.at[:, pl.ds(pl.multiple_of(k * span, span), span)]
        return pltpu.make_async_copy(scales.at[k], target, scale_sem.at[k])

    def scaled(k):
        wait_peaks(k, peak_recv)
        scale = jnp.max(peaks[k], axis=0)
        scales[k] = scale

        @pl.loop(0, depth // block)
        def _(b):
            rows = pl.ds(pl.multiple_of(b * block, block), block)
            narrow[k, rows] = (one[k, rows] / scale).astype(jnp.bfloat16)

        source = narrow.at[k]

        @pl.when(has_below)
        def _():
            whole_or_rest(k, chip == 1, lambda cut: go_down(k, 0, source, cut).start())

        @pl.when(has_above)
        def _():
            whole_or_rest(k, chip == chips - 2, lambda cut: go_up(k, 0, source, cut).start())

        go_side(k, 0, source).start()
        keep(k).start()
        keep_scale(k).start()

    lag = min(4, parts)
    zero = jnp.int32(0)
    peaks[0, me] = mixed(zero)
    pl.semaphore_wait(barrier, ranks + widths - 2)
    send_peaks(0, me, 1)

    def send_head(to):
        return pltpu.make_async_remote_copy(
            src_ref=one.at[0, pl.ds(0, taken)],
            dst_ref=head,
            send_sem=head_send,
            recv_sem=head_recv,
            device_id={"rows": to},
            device_id_type=MESH,
        )

    near_end = (chip == 1) | (chip == chips - 2)
    at_end = (chip == 0) | (chip == chips - 1)
    near_rank = jnp.where(chip == 0, me + CORES, me - CORES)

    @pl.when(near_end)
    def _():
        send_head(jnp.where(chip == 1, me - CORES, me + CORES)).start()

    def local(k):
        pairs[k, core] = mixed(k)
        pair(k).start()

    def cross(k):
        pair(k).wait_recv()
        peaks[k, chip] = jnp.max(pairs[k], axis=0)
        send_peaks(k, chip, CORES)

    def advance(k):
        local(k)
        cross(k)

    pl.loop(1, lag)(local)
    pl.loop(1, lag)(cross)
    scaled(zero)

    def head_slot():
        return slot(jnp.int32(0), near_rank).at[pl.ds(0, taken)]

    def keep_head():
        return pltpu.make_async_copy(narrow_head, head_slot(), head_out)

    @pl.when(at_end)
    def _():
        send_head(near_rank).wait_recv()
        narrow_head[...] = (head[...] / scales[0]).astype(jnp.bfloat16)
        keep_head().start()
        hop = jnp.where(chip == 0, 1, -1)
        index = hop + chips - 1
        pltpu.make_async_remote_copy(
            src_ref=narrow_head,
            dst_ref=head_slot(),
            send_sem=side_send.at[index, 0],
            recv_sem=side_recv.at[index, 0],
            device_id={"rows": partner},
            device_id_type=MESH,
        ).start()

    @pl.loop(lag, parts)
    def _(k):
        advance(k)
        scaled(k - lag + 1)

    advance(parts)
    advance(parts + 1)

    @pl.loop(1, ranks)
    def _(step):
        pltpu.make_async_remote_copy(
            src_ref=norms.at[across, me],
            dst_ref=norms.at[across, me],
            send_sem=norm_send,
            recv_sem=norm_recv,
            device_id={"rows": lax.rem(me + step, ranks)},
            device_id_type=MESH,
        ).start()

    pl.loop(parts - lag + 1, parts)(scaled)
    scaled(parts)
    scaled(parts + 1)

    others = norms.at[across, pl.ds(0, ranks - 1)]
    pltpu.make_async_copy(others, others, norm_recv).wait()

    @pl.loop(1, widths)
    def _(step):
        pltpu.make_async_remote_copy(
            src_ref=norms.at[across],
            dst_ref=norms.at[across],
            send_sem=wide_send,
            recv_sem=wide_recv,
            device_id={"width": lax.rem(across + step, widths)},
            device_id_type=MESH,
        ).start()

    def far_copies(k, rank):
        source, at = slot(k, rank), far_sem.at[k - last]
        if k <= parts:
            if k == last:
                target = far_early
            elif k == parts:
                target = far_key
            else:
                target = far_query.at[:, pl.ds((k - early) * span, span)]
            return [pltpu.make_async_copy(source, target, at)]
        most = far_value.shape[0]
        return [
            pltpu.make_async_copy(source.at[pl.ds(0, most)], far_value, at),
            pltpu.make_async_copy(
                source.at[pl.ds(most, depth - most)], far_rest, far_sem.at[k - last + 1]
            ),
        ]

    def last_early(rank, to):
        return pltpu.make_async_remote_copy(
            src_ref=slot(last, rank),
            dst_ref=far_early,
            send_sem=early_send,
            recv_sem=early_recv,
            device_id={"rows": to},
            device_id_type=MESH,
        )

    def relay(k, hop):
        is_far = is_static(k)
        is_last = is_static(k) and k == last
        onward = hop < (chips - 2 if is_last else hops(k))

        @pl.when(chip >= hop)
        def _():
            headed = (chip == chips - 1) & (hop == 1)
            whole_or_rest(k, headed, lambda cut: from_below(k, hop - 1, cut).wait_recv())

            @pl.when(has_above & onward)
            def _():
                go_up(k, hop).start()

            whole_or_rest(k, headed, lambda cut: go_side(k, -hop, None, cut).start())

            if is_last:

                @pl.when((hop == chips - 2) & has_above & (core == 1))
                def _():
                    last_early(me - CORES * hop, me + CORES).start()

            if is_far:

                @pl.when((hop == chips - 2) & (chip == chips - 2))
                def _():
                    for copy in far_copies(k, me - CORES * hop):
                        copy.start()

        @pl.when(chip + hop < chips)
        def _():
            headed = (chip == 0) & (hop == 1)
            whole_or_rest(k, headed, lambda cut: from_above(k, hop - 1, cut).wait_recv())

            @pl.when(has_below & onward)
            def _():
                go_down(k, hop).start()

            whole_or_rest(k, headed, lambda cut: go_side(k, hop, None, cut).start())

            if is_last:

                @pl.when((hop == chips - 2) & has_below & (core == 1))
                def _():
                    last_early(me + CORES * hop, me - CORES).start()

            if is_far:

                @pl.when((hop == chips - 2) & (chip == 1))
                def _():
                    for copy in far_copies(k, me + CORES * hop):
                        copy.start()

    @pl.loop(1, chips - 1)
    def _(hop):
        pl.loop(0, last)(lambda k: relay(k, hop))
        relay(last, hop)
        for k in late_parts:
            relay(k, hop)

    def finish(k):
        keep(k).wait()
        keep_scale(k).wait()
        most = chips - 2 if is_static(k) else chips - 1

        @pl.loop(0, most)
        def _(hop):
            @pl.when((chip >= hop) & has_above)
            def _():
                headed = (chip == chips - 2) & (hop == 0)
                whole_or_rest(k, headed, lambda cut: go_up(k, hop, None, cut).wait_send())

            @pl.when((chip + hop < chips) & has_below)
            def _():
                headed = (chip == 1) & (hop == 0)
                whole_or_rest(k, headed, lambda cut: go_down(k, hop, None, cut).wait_send())

        @pl.loop(0, chips)
        def _(origin):
            @pl.when((origin - chip <= most) & (chip - origin <= most))
            def _():
                go_side(k, origin - chip).wait_send()
                from_side(k, origin - chip).wait_recv()

    def settle(k):
        wait_peaks(k, peak_send)
        pl.when(k > 0)(lambda: pair(k).wait_send())

    for k in (last, *late_parts):
        finish(k)

        @pl.when(near_end)
        def _():
            for copy in far_copies(k, me):
                copy.wait()

    @pl.when(near_end)
    def _():
        send_head(partner).wait_send()

    @pl.when(at_end)
    def _():
        keep_head().wait()

    pl.loop(0, parts + 2)(settle)
    pltpu.make_async_copy(others, others, norm_send).wait()
    around = norms.at[pl.ds(0, widths - 1)]
    pltpu.make_async_copy(around, around, wide_recv).wait()
    pltpu.make_async_copy(around, around, wide_send).wait()
    keep_norms = pltpu.make_async_copy(norms, all_norms, small_sem.at[3])
    keep_norms.start()
    keep_norms.wait()

    @pl.loop(0, last)
    def _(k):
        relay(k, chips - 1)

        @pl.when(k > 0)
        def _():
            finish(k - 1)

    if last > 0:
        finish(jnp.int32(last - 1))

    @pl.when(at_end & (core == 1))
    def _():
        last_early(me, partner).wait_recv()

    @pl.when(near_end & (core == 1))
    def _():
        last_early(me, partner).wait_send()


def stream(total, incoming, outgoing, ring):
    ahead = ring // 2

    def head():
        for i in range(min(ahead, total)):
            incoming(i, True)

    def body():
        @pl.loop(0, total)
        def _(i):
            incoming(i, False)
            outgoing(i).start()

            @pl.when(i + ahead < total)
            def _():
                @pl.when(i + ahead >= ring)
                def _():
                    outgoing(i + ahead - ring).wait()

                incoming(i + ahead, True)

    def drain():
        @pl.loop(max(0, total - ring), total)
        def _(i):
            outgoing(i).wait()

    return head, body, drain


def act(copy, begin):
    if begin:
        copy.start()
    else:
        copy.wait()


def settle_kernel(
    query,
    value,
    scale_key,
    scale_value,
    new_query,
    new_value,
    new_scale_key,
    new_scale_value,
    done,
    wide_buf,
    slim_buf,
    sems,
):
    ring = wide_buf.shape[0]

    def plan(source, target, buf, at):
        step = buf.shape[1]
        cols = pl.ds(0, buf.shape[2])

        def rows(i):
            return pl.ds(pl.multiple_of(i * step, step), step)

        def incoming(i, begin):
            place = lax.rem(i, ring)
            act(
                pltpu.make_async_copy(
                    source.at[rows(i), cols], buf.at[place], sems.at[at, place]
                ),
                begin,
            )

        def outgoing(i):
            place = lax.rem(i, ring)
            return pltpu.make_async_copy(
                buf.at[place], target.at[rows(i), cols], sems.at[at + 1, place]
            )

        return stream(source.shape[0] // step, incoming, outgoing, ring)

    first = plan(query, new_query, wide_buf, 0)
    second = plan(value, new_value, slim_buf, 2)
    first[0]()
    first[1]()
    second[0]()
    second[1]()
    first[2]()
    second[2]()
    new_scale_key[...] = scale_key[...]
    new_scale_value[...] = scale_value[...]
    done[...] = jnp.zeros_like(done)


def chunk_of(rows, most):
    step = rows
    while step > most and step % 32 == 0:
        step //= 2
    return step


def settled(query, value, scale_key, scale_value, wide, ring=8):
    rows, span = value.shape
    step = chunk_of(rows, 256)
    slim = chunk_of(rows, 512)
    anywhere = pl.BlockSpec(memory_space=pl.ANY)
    near = pl.BlockSpec(memory_space=pltpu.VMEM)
    moved = 4 * rows * (wide + span)
    return pl.pallas_call(
        settle_kernel,
        out_shape=(
            jax.ShapeDtypeStruct(query.shape, query.dtype),
            jax.ShapeDtypeStruct(value.shape, value.dtype),
            jax.ShapeDtypeStruct(scale_key.shape, scale_key.dtype),
            jax.ShapeDtypeStruct(scale_value.shape, scale_value.dtype),
            jax.ShapeDtypeStruct((8, LANES), jnp.float32),
        ),
        in_specs=[anywhere, anywhere, near, near],
        out_specs=(anywhere, anywhere, near, near, near),
        scratch_shapes=[
            pltpu.VMEM((ring, step, wide), query.dtype),
            pltpu.VMEM((ring, slim, span), value.dtype),
            pltpu.SemaphoreType.DMA((4, ring)),
        ],
        compiler_params=pltpu.CompilerParams(vmem_limit_bytes=60 * 2**20),
        cost_estimate=pl.CostEstimate(
            flops=0, bytes_accessed=moved, transcendentals=0
        ),
    )(query, value, scale_key, scale_value)


def far_ranks(ranks):
    chips = ranks // CORES
    me = lax.axis_index("rows")
    chip, core = me // CORES, me % CORES
    at_end = (chip == 0) | (chip == chips - 1)
    away = jnp.where(chip == 0, chips - 1, 0) * CORES
    return at_end, away + core, away + 1 - core


def blend_kernel(ranks, first, fresh, whole, got0, got1, side0, side1, done, target, buf, sems):
    at_end, straight, crossed = far_ranks(ranks)
    core = lax.axis_index("rows") % CORES
    ring, depth, span = buf.shape
    cols = pl.ds(first, span)

    def rows(i):
        return pl.ds(pl.multiple_of(i * depth, depth), depth)

    def incoming(i, begin):
        place = lax.rem(i, ring)

        def copy(origin):
            act(pltpu.make_async_copy(origin, buf.at[place], sems.at[0, place]), begin)

        if not begin:
            copy(whole.at[rows(i), cols])
            return
        is_got = at_end & (i == straight)
        is_side = at_end & (i == crossed)
        pl.when(is_got & (core == 0))(lambda: copy(got0))
        pl.when(is_got & (core == 1))(lambda: copy(got1))
        pl.when(is_side & (core == 0))(lambda: copy(side0))
        pl.when(is_side & (core == 1))(lambda: copy(side1))
        pl.when(jnp.logical_not(is_got | is_side))(lambda: copy(whole.at[rows(i), cols]))

    def outgoing(i):
        place = lax.rem(i, ring)
        return pltpu.make_async_copy(
            buf.at[place], target.at[rows(i), cols], sems.at[1, place]
        )

    for phase in stream(ranks, incoming, outgoing, ring):
        phase()


def blended(ranks, first, fresh, whole, gots, sides, done, ring=6):
    anywhere = pl.BlockSpec(memory_space=pl.ANY)
    return pl.pallas_call(
        functools.partial(blend_kernel, ranks, first),
        out_shape=jax.ShapeDtypeStruct(whole.shape, whole.dtype),
        in_specs=[anywhere] * 7,
        out_specs=anywhere,
        scratch_shapes=[
            pltpu.VMEM((ring, *gots[0].shape), whole.dtype),
            pltpu.SemaphoreType.DMA((2, ring)),
        ],
        input_output_aliases={} if fresh is done else {0: 0},
        compiler_params=pltpu.CompilerParams(vmem_limit_bytes=60 * 2**20),
        cost_estimate=pl.CostEstimate(
            flops=0, bytes_accessed=4 * ranks * gots[0].size, transcendentals=0
        ),
    )(fresh, whole, *gots, *sides, done)


def place_kernel(ranks, depth, _, *refs):
    gots, sides, (target, sems) = refs[0:2], refs[2:4], refs[4:]
    at_end, straight, crossed = far_ranks(ranks)

    @pl.when(at_end)
    def _():
        copies = []
        for rank, pieces in ((straight, gots), (crossed, sides)):
            row = rank * depth
            for piece in pieces:
                rows = pl.ds(pl.multiple_of(row, 8), piece.shape[0])
                at = sems.at[len(copies)]
                copies.append(pltpu.make_async_copy(piece, target.at[rows], at))
                row = row + piece.shape[0]
        for copy in copies:
            copy.start()
        for copy in copies:
            copy.wait()


def placed(ranks, whole, gots, sides):
    anywhere = pl.BlockSpec(memory_space=pl.ANY)
    near = pl.BlockSpec(memory_space=pltpu.VMEM)
    depth = whole.shape[0] // ranks
    return pl.pallas_call(
        functools.partial(place_kernel, ranks, depth),
        out_shape=jax.ShapeDtypeStruct(whole.shape, whole.dtype),
        in_specs=[anywhere, near, near, near, near],
        out_specs=anywhere,
        scratch_shapes=[pltpu.SemaphoreType.DMA((4,))],
        input_output_aliases={0: 0},
        compiler_params=pltpu.CompilerParams(vmem_limit_bytes=8 * 2**20),
        cost_estimate=pl.CostEstimate(
            flops=0, bytes_accessed=8 * gots[0].size, transcendentals=0
        ),
    )(whole, *gots, *sides)


def shards(
    ranks,
    widths,
    one_query,
    other_query,
    one_key,
    other_key,
    one_value,
    other_value,
    mix_share,
    norm_train,
    norm_step,
):
    depth, span = one_key.shape
    wide = one_query.shape[1]
    parts = wide // span
    chips = ranks // CORES
    bit = norm_train.shape[0]
    late = LATE * span
    tail = max(8, depth // 32 * 8)
    head = min(HEAD, depth // 16 * 8)
    tall = -(-depth // LANES) * LANES
    if tall != depth:
        mix_share = jnp.pad(mix_share, (0, tall - depth))
    mix_rows = mix_share.reshape(tall // LANES, LANES)
    shape = jax.ShapeDtypeStruct
    anywhere = pl.BlockSpec(memory_space=pl.ANY)
    dma = pltpu.SemaphoreType.DMA
    (
        query, key, value, far_early, far_query, far_key, far_value, far_rest,
        scale_query, scale_key, scale_value, norms,
    ) = pl.pallas_call(
        functools.partial(merge, ranks, widths),
        out_shape=(
            shape((ranks * depth, wide), jnp.bfloat16),
            shape((ranks * depth, span), jnp.bfloat16),
            shape((ranks * depth, span), jnp.bfloat16),
            shape((depth, span), jnp.bfloat16),
            shape((depth, late), jnp.bfloat16),
            shape((depth, span), jnp.bfloat16),
            shape((depth - tail, span), jnp.bfloat16),
            shape((tail, span), jnp.bfloat16),
            shape((1, wide), jnp.float32),
            shape((1, span), jnp.float32),
            shape((1, span), jnp.float32),
            shape((widths, ranks, 1, bit), jnp.float32),
        ),
        in_specs=[anywhere] * 9,
        out_specs=[anywhere] * 12,
        scratch_shapes=[
            pltpu.VMEM((parts + 2, depth, span), jnp.float32),
            pltpu.VMEM((parts + 2, depth, span), jnp.float32),
            pltpu.VMEM((parts + 2, depth, span), jnp.bfloat16),
            pltpu.VMEM(mix_rows.shape, jnp.float32),
            pltpu.VMEM((tall, LANES), jnp.float32),
            pltpu.VMEM((2, 1, bit), jnp.float32),
            pltpu.VMEM((widths, ranks, 1, bit), jnp.float32),
            pltpu.VMEM((parts + 2, 1, span), jnp.float32),
            pltpu.VMEM((parts + 2, CORES, 1, span), jnp.float32),
            pltpu.VMEM((parts + 2, ranks, 1, span), jnp.float32),
            pltpu.VMEM((head, span), jnp.float32),
            pltpu.VMEM((head, span), jnp.bfloat16),
            dma((4,)),
            dma((2, parts + 2)),
            dma((parts + 2,)),
            dma((parts + 2,)),
            dma((LATE + 4,)),
            dma((parts + 2,)),
            dma((parts + 2,)),
            dma((parts + 2,)),
            dma((parts + 2,)),
            dma,
            dma,
            dma,
            dma,
            dma((chips - 1, parts + 2)),
            dma((chips - 1, parts + 2)),
            dma((chips - 1, parts + 2)),
            dma((chips - 1, parts + 2)),
            dma((2 * chips - 1, parts + 2)),
            dma((2 * chips - 1, parts + 2)),
            dma,
            dma,
            dma,
            dma,
            dma,
        ],
        compiler_params=pltpu.CompilerParams(
            collective_id=0, has_side_effects=True, vmem_limit_bytes=56 * 2**20
        ),
    )(
        one_query,
        other_query,
        one_key,
        other_key,
        one_value,
        other_value,
        mix_rows,
        norm_train[None],
        norm_step[None],
    )
    first = wide - late - span
    ends = ((1, 0), (chips - 2, chips - 1))

    def send(piece, *pairs):
        return lax.ppermute(
            piece,
            "rows",
            [
                (source * CORES + a, target * CORES + b)
                for near, end in ends
                for hop in pairs
                for (source, a), (target, b) in [
                    ((near if hop[0] else end, hop[1]), (end, hop[2]))
                ]
            ],
        )

    def last_hop(piece):
        return send(piece, (True, 0, 0), (True, 1, 1))

    def to_side(piece):
        return send(piece, (False, 0, 1), (False, 1, 0))

    got_early = send(far_early, (True, 0, 0))
    got_query = last_hop(far_query)
    got_key = last_hop(far_key)
    got_value = last_hop(far_value)
    got_rest = last_hop(far_rest)
    new_query, new_value, scale_key, scale_value, done = settled(
        query, value, scale_key, scale_value, first
    )
    small = (
        scale_query[0],
        scale_key[0],
        scale_value[0],
        norms.transpose(1, 0, 2, 3).reshape(-1).astype(jnp.bfloat16),
    )
    got_early, far_early, done = lax.optimization_barrier((got_early, far_early, done))
    sides = send(far_early, (False, 1, 0)), send(got_early, (False, 0, 1))
    new_query = blended(
        ranks, first, new_query, query, (got_early, far_early), sides, done
    )
    got_query, new_query = lax.optimization_barrier((got_query, new_query))
    new_query = blended(
        ranks, first + span, new_query, query, [got_query] * 2, [to_side(got_query)] * 2, done
    )
    got_key, new_query = lax.optimization_barrier((got_key, new_query))
    new_key = blended(ranks, 0, done, key, [got_key] * 2, [to_side(got_key)] * 2, done)
    got_value, new_key, small = lax.optimization_barrier((got_value, new_key, small))
    sides = to_side(got_value), to_side(got_rest)
    new_value = placed(ranks, new_value, (got_value, got_rest), sides)
    return (new_query, new_key, new_value, *small)


def solution(mesh):
    in_specs = (
        P(("site", "rows"), "width"),
        P(("site", "rows"), "width"),
        P(("site", "rows"), "width"),
        P(("site", "rows"), "width"),
        P(("site", "rows"), "width"),
        P(("site", "rows"), "width"),
        P(("site", "rows")),
        P(("site", "rows", "width")),
        P(("site", "rows", "width")),
    )
    out_specs = (
        P("site", "width"),
        P("site", "width"),
        P("site", "width"),
        P(("site", "width")),
        P(("site", "width")),
        P(("site", "width")),
        P("site"),
    )
    body = functools.partial(shards, mesh.shape["rows"], mesh.shape["width"])

    return jax.shard_map(
        body, mesh=mesh, in_specs=in_specs, out_specs=out_specs, check_vma=False
    )
```

```python
import functools

import jax
import jax.numpy as jnp
from jax import lax
from jax.experimental import pallas as pl
from jax.experimental.pallas import tpu as pltpu
from jax.sharding import PartitionSpec as P


MESH = pl.DeviceIdType.MESH
CORES = 2
LANES = 128
LATE = 2
AHEAD = 3
HEAD = 96


def merge(
    ranks,
    widths,
    one_query,
    other_query,
    one_key,
    other_key,
    one_value,
    other_value,
    mix_share,
    norm_train,
    norm_step,
    query,
    key,
    value,
    far_early,
    far_query,
    far_key,
    far_value,
    far_rest,
    scale_query,
    scale_key,
    scale_value,
    all_norms,
    one,
    other,
    narrow,
    mix_row,
    mix,
    steps,
    norms,
    scales,
    pairs,
    peaks,
    head,
    narrow_head,
    small_sem,
    load_sem,
    out_sem,
    scale_sem,
    far_sem,
    pair_send,
    pair_recv,
    peak_send,
    peak_recv,
    norm_send,
    norm_recv,
    wide_send,
    wide_recv,
    up_send,
    up_recv,
    down_send,
    down_recv,
    side_send,
    side_recv,
    early_send,
    early_recv,
    head_send,
    head_recv,
    head_out,
):
    depth, span = one_key.shape
    parts = one_query.shape[1] // span
    early = parts - LATE
    chips = ranks // CORES
    me = lax.axis_index("rows")
    across = lax.axis_index("width")
    chip, core = me // CORES, me % CORES
    partner = chip * CORES + 1 - core
    last = early - 1
    block = 32 if depth % 32 == 0 else depth
    late_parts = range(early, parts + 2)
    taken = head.shape[0]
    rest = pl.ds(taken, depth - taken)

    def is_static(k):
        return isinstance(k, int)

    def loads(k):
        if is_static(k) and k >= parts:
            sources = (one_key, other_key) if k == parts else (one_value, other_value)
        else:
            cut = pl.ds(pl.multiple_of(k * span, span), span)
            sources = one_query.at[:, cut], other_query.at[:, cut]
        return [
            pltpu.make_async_copy(source, target.at[k], load_sem.at[i, k])
            for i, (source, target) in enumerate(zip(sources, (one, other)))
        ]

    def load(k):
        for copy in loads(k):
            copy.start()

    barrier = pltpu.get_barrier_semaphore()

    @pl.loop(1, ranks)
    def _(step):
        to = {"rows": lax.rem(me + step, ranks)}
        pl.semaphore_signal(barrier, inc=1, device_id=to, device_id_type=MESH)

    @pl.loop(1, widths)
    def _(step):
        to = {"width": lax.rem(across + step, widths)}
        pl.semaphore_signal(barrier, inc=1, device_id=to, device_id_type=MESH)

    small = [
        pltpu.make_async_copy(mix_share, mix_row, small_sem.at[0]),
        pltpu.make_async_copy(norm_train, steps.at[0], small_sem.at[1]),
        pltpu.make_async_copy(norm_step, steps.at[1], small_sem.at[2]),
    ]
    for copy in small:
        copy.start()

    pl.loop(0, AHEAD)(load)

    for copy in small:
        copy.wait()
    norms[across, me] = steps[0] + steps[1]

    for i in range(mix_row.shape[0]):
        row = jnp.broadcast_to(mix_row[i : i + 1], (LANES, LANES))
        mix[i * LANES : (i + 1) * LANES] = row.T

    peaks[1:, chips:] = jnp.zeros((parts + 1, ranks - chips, 1, span), jnp.float32)

    def send_peaks(k, mine, stride):
        @pl.loop(1, ranks // stride)
        def _(step):
            pltpu.make_async_remote_copy(
                src_ref=peaks.at[k, mine],
                dst_ref=peaks.at[k, mine],
                send_sem=peak_send.at[k],
                recv_sem=peak_recv.at[k],
                device_id={"rows": lax.rem(me + stride * step, ranks)},
                device_id_type=MESH,
            ).start()

    def wait_peaks(k, sem):
        def wait(count):
            everyone = peaks.at[k, pl.ds(0, count)]
            pltpu.make_async_copy(everyone, everyone, sem.at[k]).wait()

        if is_static(k):
            wait(chips - 1 if k else ranks - 1)
            return
        pl.when(k == 0)(lambda: wait(ranks - 1))
        pl.when(k > 0)(lambda: wait(chips - 1))

    def pair(k):
        return pltpu.make_async_remote_copy(
            src_ref=pairs.at[k, core],
            dst_ref=pairs.at[k, core],
            send_sem=pair_send.at[k],
            recv_sem=pair_recv.at[k],
            device_id={"rows": partner},
            device_id_type=MESH,
        )

    def mixed(k):
        for copy in loads(k):
            copy.wait()
        if is_static(k):
            if k + AHEAD < parts + 2:
                load(k + AHEAD)
        else:

            @pl.when(k + AHEAD < parts)
            def _():
                load(k + AHEAD)

            for tail in (parts, parts + 1):

                @pl.when(k + AHEAD == tail)
                def _():
                    load(tail)

        def step(b, top):
            rows = pl.ds(pl.multiple_of(b * block, block), block)
            share = jnp.concatenate([mix[rows]] * (span // LANES), axis=1)
            whole = share * one[k, rows] + (1.0 - share) * other[k, rows]
            one[k, rows] = whole
            return jnp.maximum(top, jnp.max(jnp.abs(whole).reshape(-1, 8, span), axis=0))

        top = lax.fori_loop(0, depth // block, step, jnp.zeros((8, span), jnp.float32))
        return jnp.max(top, axis=0, keepdims=True)

    def is_tail(k):
        return is_static(k) and k >= parts

    def hops(k):
        return chips - 2 if is_static(k) and k >= early else chips - 1

    def slot(k, rank):
        rows = pl.ds(pl.multiple_of(rank * depth, depth), depth)
        if is_tail(k):
            return (key if k == parts else value).at[rows]
        return query.at[rows, pl.ds(pl.multiple_of(k * span, span), span)]

    def send(k, rank, to, send_sem, recv_sem, source=None, cut=None):
        target = slot(k, rank)
        source = target if source is None else source
        if cut is not None:
            source, target = source.at[cut], target.at[cut]
        return pltpu.make_async_remote_copy(
            src_ref=source,
            dst_ref=target,
            send_sem=send_sem,
            recv_sem=recv_sem,
            device_id={"rows": to},
            device_id_type=MESH,
        )

    def go_up(k, hop, source=None, cut=None):
        sems = up_send.at[hop, k], up_recv.at[hop, k]
        return send(k, me - CORES * hop, me + CORES, *sems, source, cut)

    def go_down(k, hop, source=None, cut=None):
        sems = down_send.at[hop, k], down_recv.at[hop, k]
        return send(k, me + CORES * hop, me - CORES, *sems, source, cut)

    def go_side(k, hop, source=None, cut=None):
        index = hop + chips - 1
        sems = side_send.at[index, k], side_recv.at[index, k]
        return send(k, me + CORES * hop, partner, *sems, source, cut)

    def from_side(k, hop):
        index = hop + chips - 1
        return send(
            k, partner + CORES * hop, partner, side_send.at[index, k], side_recv.at[index, k]
        )

    def from_below(k, hop, cut=None):
        sems = up_send.at[hop, k], up_recv.at[hop, k]
        return send(k, me - CORES * (hop + 1), me - CORES, *sems, None, cut)

    def from_above(k, hop, cut=None):
        sems = down_send.at[hop, k], down_recv.at[hop, k]
        return send(k, me + CORES * (hop + 1), me + CORES, *sems, None, cut)

    def whole_or_rest(k, headed, action):
        if is_static(k):
            action(None)
            return
        headed = headed & (k == 0)
        pl.when(headed)(lambda: action(rest))
        pl.when(jnp.logical_not(headed))(lambda: action(None))

    has_below, has_above = chip >= 1, chip < chips - 1

    def keep(k):
        return pltpu.make_async_copy(narrow.at[k], slot(k, me), out_sem.at[k])

    def keep_scale(k):
        if is_tail(k):
            target = scale_key if k == parts else scale_value
        else:
            target = scale_query.at[:, pl.ds(pl.multiple_of(k * span, span), span)]
        return pltpu.make_async_copy(scales.at[k], target, scale_sem.at[k])

    def scaled(k):
        wait_peaks(k, peak_recv)
        scale = jnp.max(peaks[k], axis=0)
        scales[k] = scale

        @pl.loop(0, depth // block)
        def _(b):
            rows = pl.ds(pl.multiple_of(b * block, block), block)
            narrow[k, rows] = (one[k, rows] / scale).astype(jnp.bfloat16)

        source = narrow.at[k]

        @pl.when(has_below)
        def _():
            whole_or_rest(k, chip == 1, lambda cut: go_down(k, 0, source, cut).start())

        @pl.when(has_above)
        def _():
            whole_or_rest(k, chip == chips - 2, lambda cut: go_up(k, 0, source, cut).start())

        go_side(k, 0, source).start()
        keep(k).start()
        keep_scale(k).start()

    lag = min(4, parts)
    zero = jnp.int32(0)
    peaks[0, me] = mixed(zero)
    pl.semaphore_wait(barrier, ranks + widths - 2)
    send_peaks(0, me, 1)

    def send_head(to):
        return pltpu.make_async_remote_copy(
            src_ref=one.at[0, pl.ds(0, taken)],
            dst_ref=head,
            send_sem=head_send,
            recv_sem=head_recv,
            device_id={"rows": to},
            device_id_type=MESH,
        )

    near_end = (chip == 1) | (chip == chips - 2)
    at_end = (chip == 0) | (chip == chips - 1)
    near_rank = jnp.where(chip == 0, me + CORES, me - CORES)

    @pl.when(near_end)
    def _():
        send_head(jnp.where(chip == 1, me - CORES, me + CORES)).start()

    def local(k):
        pairs[k, core] = mixed(k)
        pair(k).start()

    def cross(k):
        pair(k).wait_recv()
        peaks[k, chip] = jnp.max(pairs[k], axis=0)
        send_peaks(k, chip, CORES)

    def advance(k):
        local(k)
        cross(k)

    pl.loop(1, lag)(local)
    pl.loop(1, lag)(cross)
    scaled(zero)

    def head_slot():
        return slot(jnp.int32(0), near_rank).at[pl.ds(0, taken)]

    def keep_head():
        return pltpu.make_async_copy(narrow_head, head_slot(), head_out)

    @pl.when(at_end)
    def _():
        send_head(near_rank).wait_recv()
        narrow_head[...] = (head[...] / scales[0]).astype(jnp.bfloat16)
        keep_head().start()
        hop = jnp.where(chip == 0, 1, -1)
        index = hop + chips - 1
        pltpu.make_async_remote_copy(
            src_ref=narrow_head,
            dst_ref=head_slot(),
            send_sem=side_send.at[index, 0],
            recv_sem=side_recv.at[index, 0],
            device_id={"rows": partner},
            device_id_type=MESH,
        ).start()

    @pl.loop(lag, parts)
    def _(k):
        advance(k)
        scaled(k - lag + 1)

    advance(parts)
    advance(parts + 1)

    @pl.loop(1, ranks)
    def _(step):
        pltpu.make_async_remote_copy(
            src_ref=norms.at[across, me],
            dst_ref=norms.at[across, me],
            send_sem=norm_send,
            recv_sem=norm_recv,
            device_id={"rows": lax.rem(me + step, ranks)},
            device_id_type=MESH,
        ).start()

    pl.loop(parts - lag + 1, parts)(scaled)
    scaled(parts)
    scaled(parts + 1)

    others = norms.at[across, pl.ds(0, ranks - 1)]
    pltpu.make_async_copy(others, others, norm_recv).wait()

    @pl.loop(1, widths)
    def _(step):
        pltpu.make_async_remote_copy(
            src_ref=norms.at[across],
            dst_ref=norms.at[across],
            send_sem=wide_send,
            recv_sem=wide_recv,
            device_id={"width": lax.rem(across + step, widths)},
            device_id_type=MESH,
        ).start()

    def far_copies(k, rank):
        source, at = slot(k, rank), far_sem.at[k - last]
        if k <= parts:
            if k == last:
                target = far_early
            elif k == parts:
                target = far_key
            else:
                target = far_query.at[:, pl.ds((k - early) * span, span)]
            return [pltpu.make_async_copy(source, target, at)]
        most = far_value.shape[0]
        return [
            pltpu.make_async_copy(source.at[pl.ds(0, most)], far_value, at),
            pltpu.make_async_copy(
                source.at[pl.ds(most, depth - most)], far_rest, far_sem.at[k - last + 1]
            ),
        ]

    def last_early(rank, to):
        return pltpu.make_async_remote_copy(
            src_ref=slot(last, rank),
            dst_ref=far_early,
            send_sem=early_send,
            recv_sem=early_recv,
            device_id={"rows": to},
            device_id_type=MESH,
        )

    def relay(k, hop):
        is_far = is_static(k)
        is_last = is_static(k) and k == last
        onward = hop < (chips - 2 if is_last else hops(k))

        @pl.when(chip >= hop)
        def _():
            headed = (chip == chips - 1) & (hop == 1)
            whole_or_rest(k, headed, lambda cut: from_below(k, hop - 1, cut).wait_recv())

            @pl.when(has_above & onward)
            def _():
                go_up(k, hop).start()

            whole_or_rest(k, headed, lambda cut: go_side(k, -hop, None, cut).start())

            if is_last:

                @pl.when((hop == chips - 2) & has_above & (core == 1))
                def _():
                    last_early(me - CORES * hop, me + CORES).start()

            if is_far:

                @pl.when((hop == chips - 2) & (chip == chips - 2))
                def _():
                    for copy in far_copies(k, me - CORES * hop):
                        copy.start()

        @pl.when(chip + hop < chips)
        def _():
            headed = (chip == 0) & (hop == 1)
            whole_or_rest(k, headed, lambda cut: from_above(k, hop - 1, cut).wait_recv())

            @pl.when(has_below & onward)
            def _():
                go_down(k, hop).start()

            whole_or_rest(k, headed, lambda cut: go_side(k, hop, None, cut).start())

            if is_last:

                @pl.when((hop == chips - 2) & has_below & (core == 1))
                def _():
                    last_early(me + CORES * hop, me - CORES).start()

            if is_far:

                @pl.when((hop == chips - 2) & (chip == 1))
                def _():
                    for copy in far_copies(k, me + CORES * hop):
                        copy.start()

    @pl.loop(1, chips - 1)
    def _(hop):
        pl.loop(0, last)(lambda k: relay(k, hop))
        relay(last, hop)
        for k in late_parts:
            relay(k, hop)

    def finish(k):
        keep(k).wait()
        keep_scale(k).wait()
        most = chips - 2 if is_static(k) else chips - 1

        @pl.loop(0, most)
        def _(hop):
            @pl.when((chip >= hop) & has_above)
            def _():
                headed = (chip == chips - 2) & (hop == 0)
                whole_or_rest(k, headed, lambda cut: go_up(k, hop, None, cut).wait_send())

            @pl.when((chip + hop < chips) & has_below)
            def _():
                headed = (chip == 1) & (hop == 0)
                whole_or_rest(k, headed, lambda cut: go_down(k, hop, None, cut).wait_send())

        @pl.loop(0, chips)
        def _(origin):
            @pl.when((origin - chip <= most) & (chip - origin <= most))
            def _():
                go_side(k, origin - chip).wait_send()
                from_side(k, origin - chip).wait_recv()

    def settle(k):
        wait_peaks(k, peak_send)
        pl.when(k > 0)(lambda: pair(k).wait_send())

    for k in (last, *late_parts):
        finish(k)

        @pl.when(near_end)
        def _():
            for copy in far_copies(k, me):
                copy.wait()

    @pl.when(near_end)
    def _():
        send_head(partner).wait_send()

    @pl.when(at_end)
    def _():
        keep_head().wait()

    pl.loop(0, parts + 2)(settle)
    pltpu.make_async_copy(others, others, norm_send).wait()
    around = norms.at[pl.ds(0, widths - 1)]
    pltpu.make_async_copy(around, around, wide_recv).wait()
    pltpu.make_async_copy(around, around, wide_send).wait()
    keep_norms = pltpu.make_async_copy(norms, all_norms, small_sem.at[3])
    keep_norms.start()
    keep_norms.wait()

    @pl.loop(0, last)
    def _(k):
        relay(k, chips - 1)

        @pl.when(k > 0)
        def _():
            finish(k - 1)

    if last > 0:
        finish(jnp.int32(last - 1))

    @pl.when(at_end & (core == 1))
    def _():
        last_early(me, partner).wait_recv()

    @pl.when(near_end & (core == 1))
    def _():
        last_early(me, partner).wait_send()


def stream(total, incoming, outgoing, ring):
    ahead = ring // 2

    def head():
        for i in range(min(ahead, total)):
            incoming(i, True)

    def body():
        @pl.loop(0, total)
        def _(i):
            incoming(i, False)
            outgoing(i).start()

            @pl.when(i + ahead < total)
            def _():
                @pl.when(i + ahead >= ring)
                def _():
                    outgoing(i + ahead - ring).wait()

                incoming(i + ahead, True)

    def drain():
        @pl.loop(max(0, total - ring), total)
        def _(i):
            outgoing(i).wait()

    return head, body, drain


def act(copy, begin):
    if begin:
        copy.start()
    else:
        copy.wait()


def settle_kernel(
    query,
    value,
    scale_key,
    scale_value,
    new_query,
    new_value,
    new_scale_key,
    new_scale_value,
    done,
    wide_buf,
    slim_buf,
    sems,
):
    ring = wide_buf.shape[0]

    def plan(source, target, buf, at):
        step = buf.shape[1]
        cols = pl.ds(0, buf.shape[2])

        def rows(i):
            return pl.ds(pl.multiple_of(i * step, step), step)

        def incoming(i, begin):
            place = lax.rem(i, ring)
            act(
                pltpu.make_async_copy(
                    source.at[rows(i), cols], buf.at[place], sems.at[at, place]
                ),
                begin,
            )

        def outgoing(i):
            place = lax.rem(i, ring)
            return pltpu.make_async_copy(
                buf.at[place], target.at[rows(i), cols], sems.at[at + 1, place]
            )

        return stream(source.shape[0] // step, incoming, outgoing, ring)

    first = plan(query, new_query, wide_buf, 0)
    second = plan(value, new_value, slim_buf, 2)
    first[0]()
    first[1]()
    second[0]()
    second[1]()
    first[2]()
    second[2]()
    new_scale_key[...] = scale_key[...]
    new_scale_value[...] = scale_value[...]
    done[...] = jnp.zeros_like(done)


def chunk_of(rows, most):
    step = rows
    while step > most and step % 32 == 0:
        step //= 2
    return step


def settled(query, value, scale_key, scale_value, wide, ring=8):
    rows, span = value.shape
    step = chunk_of(rows, 256)
    slim = chunk_of(rows, 512)
    anywhere = pl.BlockSpec(memory_space=pl.ANY)
    near = pl.BlockSpec(memory_space=pltpu.VMEM)
    moved = 4 * rows * (wide + span)
    return pl.pallas_call(
        settle_kernel,
        out_shape=(
            jax.ShapeDtypeStruct(query.shape, query.dtype),
            jax.ShapeDtypeStruct(value.shape, value.dtype),
            jax.ShapeDtypeStruct(scale_key.shape, scale_key.dtype),
            jax.ShapeDtypeStruct(scale_value.shape, scale_value.dtype),
            jax.ShapeDtypeStruct((8, LANES), jnp.float32),
        ),
        in_specs=[anywhere, anywhere, near, near],
        out_specs=(anywhere, anywhere, near, near, near),
        scratch_shapes=[
            pltpu.VMEM((ring, step, wide), query.dtype),
            pltpu.VMEM((ring, slim, span), value.dtype),
            pltpu.SemaphoreType.DMA((4, ring)),
        ],
        compiler_params=pltpu.CompilerParams(vmem_limit_bytes=60 * 2**20),
        cost_estimate=pl.CostEstimate(
            flops=0, bytes_accessed=moved, transcendentals=0
        ),
    )(query, value, scale_key, scale_value)


def far_ranks(ranks):
    chips = ranks // CORES
    me = lax.axis_index("rows")
    chip, core = me // CORES, me % CORES
    at_end = (chip == 0) | (chip == chips - 1)
    away = jnp.where(chip == 0, chips - 1, 0) * CORES
    return at_end, away + core, away + 1 - core


def blend_kernel(ranks, first, fresh, whole, got0, got1, side0, side1, done, target, buf, sems):
    at_end, straight, crossed = far_ranks(ranks)
    core = lax.axis_index("rows") % CORES
    ring, depth, span = buf.shape
    cols = pl.ds(first, span)

    def rows(i):
        return pl.ds(pl.multiple_of(i * depth, depth), depth)

    def incoming(i, begin):
        place = lax.rem(i, ring)

        def copy(origin):
            act(pltpu.make_async_copy(origin, buf.at[place], sems.at[0, place]), begin)

        if not begin:
            copy(whole.at[rows(i), cols])
            return
        is_got = at_end & (i == straight)
        is_side = at_end & (i == crossed)
        pl.when(is_got & (core == 0))(lambda: copy(got0))
        pl.when(is_got & (core == 1))(lambda: copy(got1))
        pl.when(is_side & (core == 0))(lambda: copy(side0))
        pl.when(is_side & (core == 1))(lambda: copy(side1))
        pl.when(jnp.logical_not(is_got | is_side))(lambda: copy(whole.at[rows(i), cols]))

    def outgoing(i):
        place = lax.rem(i, ring)
        return pltpu.make_async_copy(
            buf.at[place], target.at[rows(i), cols], sems.at[1, place]
        )

    for phase in stream(ranks, incoming, outgoing, ring):
        phase()


def blended(ranks, first, fresh, whole, gots, sides, done, ring=6):
    anywhere = pl.BlockSpec(memory_space=pl.ANY)
    return pl.pallas_call(
        functools.partial(blend_kernel, ranks, first),
        out_shape=jax.ShapeDtypeStruct(whole.shape, whole.dtype),
        in_specs=[anywhere] * 7,
        out_specs=anywhere,
        scratch_shapes=[
            pltpu.VMEM((ring, *gots[0].shape), whole.dtype),
            pltpu.SemaphoreType.DMA((2, ring)),
        ],
        input_output_aliases={} if fresh is done else {0: 0},
        compiler_params=pltpu.CompilerParams(vmem_limit_bytes=60 * 2**20),
        cost_estimate=pl.CostEstimate(
            flops=0, bytes_accessed=4 * ranks * gots[0].size, transcendentals=0
        ),
    )(fresh, whole, *gots, *sides, done)


def place_kernel(ranks, depth, first, _, got, side, target, sems):
    at_end, straight, crossed = far_ranks(ranks)

    @pl.when(at_end)
    def _():
        copies = []
        for at, (rank, piece) in enumerate(((straight, got), (crossed, side))):
            rows = pl.ds(pl.multiple_of(rank * depth + first, 8), piece.shape[0])
            copies.append(pltpu.make_async_copy(piece, target.at[rows], sems.at[at]))
        for copy in copies:
            copy.start()
        for copy in copies:
            copy.wait()


def placed(ranks, first, whole, got, side):
    anywhere = pl.BlockSpec(memory_space=pl.ANY)
    near = pl.BlockSpec(memory_space=pltpu.VMEM)
    depth = whole.shape[0] // ranks
    return pl.pallas_call(
        functools.partial(place_kernel, ranks, depth, first),
        out_shape=jax.ShapeDtypeStruct(whole.shape, whole.dtype),
        in_specs=[anywhere, near, near],
        out_specs=anywhere,
        scratch_shapes=[pltpu.SemaphoreType.DMA((2,))],
        input_output_aliases={0: 0},
        compiler_params=pltpu.CompilerParams(vmem_limit_bytes=8 * 2**20),
        cost_estimate=pl.CostEstimate(
            flops=0, bytes_accessed=8 * got.size, transcendentals=0
        ),
    )(whole, got, side)


def shards(
    ranks,
    widths,
    one_query,
    other_query,
    one_key,
    other_key,
    one_value,
    other_value,
    mix_share,
    norm_train,
    norm_step,
):
    depth, span = one_key.shape
    wide = one_query.shape[1]
    parts = wide // span
    chips = ranks // CORES
    bit = norm_train.shape[0]
    late = LATE * span
    tail = max(8, depth // 32 * 8)
    head = min(HEAD, depth // 16 * 8)
    tall = -(-depth // LANES) * LANES
    if tall != depth:
        mix_share = jnp.pad(mix_share, (0, tall - depth))
    mix_rows = mix_share.reshape(tall // LANES, LANES)
    shape = jax.ShapeDtypeStruct
    anywhere = pl.BlockSpec(memory_space=pl.ANY)
    dma = pltpu.SemaphoreType.DMA
    (
        query, key, value, far_early, far_query, far_key, far_value, far_rest,
        scale_query, scale_key, scale_value, norms,
    ) = pl.pallas_call(
        functools.partial(merge, ranks, widths),
        out_shape=(
            shape((ranks * depth, wide), jnp.bfloat16),
            shape((ranks * depth, span), jnp.bfloat16),
            shape((ranks * depth, span), jnp.bfloat16),
            shape((depth, span), jnp.bfloat16),
            shape((depth, late), jnp.bfloat16),
            shape((depth, span), jnp.bfloat16),
            shape((depth - tail, span), jnp.bfloat16),
            shape((tail, span), jnp.bfloat16),
            shape((1, wide), jnp.float32),
            shape((1, span), jnp.float32),
            shape((1, span), jnp.float32),
            shape((widths, ranks, 1, bit), jnp.float32),
        ),
        in_specs=[anywhere] * 9,
        out_specs=[anywhere] * 12,
        scratch_shapes=[
            pltpu.VMEM((parts + 2, depth, span), jnp.float32),
            pltpu.VMEM((parts + 2, depth, span), jnp.float32),
            pltpu.VMEM((parts + 2, depth, span), jnp.bfloat16),
            pltpu.VMEM(mix_rows.shape, jnp.float32),
            pltpu.VMEM((tall, LANES), jnp.float32),
            pltpu.VMEM((2, 1, bit), jnp.float32),
            pltpu.VMEM((widths, ranks, 1, bit), jnp.float32),
            pltpu.VMEM((parts + 2, 1, span), jnp.float32),
            pltpu.VMEM((parts + 2, CORES, 1, span), jnp.float32),
            pltpu.VMEM((parts + 2, ranks, 1, span), jnp.float32),
            pltpu.VMEM((head, span), jnp.float32),
            pltpu.VMEM((head, span), jnp.bfloat16),
            dma((4,)),
            dma((2, parts + 2)),
            dma((parts + 2,)),
            dma((parts + 2,)),
            dma((LATE + 4,)),
            dma((parts + 2,)),
            dma((parts + 2,)),
            dma((parts + 2,)),
            dma((parts + 2,)),
            dma,
            dma,
            dma,
            dma,
            dma((chips - 1, parts + 2)),
            dma((chips - 1, parts + 2)),
            dma((chips - 1, parts + 2)),
            dma((chips - 1, parts + 2)),
            dma((2 * chips - 1, parts + 2)),
            dma((2 * chips - 1, parts + 2)),
            dma,
            dma,
            dma,
            dma,
            dma,
        ],
        compiler_params=pltpu.CompilerParams(
            collective_id=0, has_side_effects=True, vmem_limit_bytes=56 * 2**20
        ),
    )(
        one_query,
        other_query,
        one_key,
        other_key,
        one_value,
        other_value,
        mix_rows,
        norm_train[None],
        norm_step[None],
    )
    first = wide - late - span
    ends = ((1, 0), (chips - 2, chips - 1))

    def send(piece, *pairs):
        return lax.ppermute(
            piece,
            "rows",
            [
                (source * CORES + a, target * CORES + b)
                for near, end in ends
                for hop in pairs
                for (source, a), (target, b) in [
                    ((near if hop[0] else end, hop[1]), (end, hop[2]))
                ]
            ],
        )

    def last_hop(piece):
        return send(piece, (True, 0, 0), (True, 1, 1))

    def to_side(piece):
        return send(piece, (False, 0, 1), (False, 1, 0))

    got_early = send(far_early, (True, 0, 0))
    got_query = last_hop(far_query)
    got_key = last_hop(far_key)
    got_value = last_hop(far_value)
    got_rest = last_hop(far_rest)
    new_query, new_value, scale_key, scale_value, done = settled(
        query, value, scale_key, scale_value, first
    )
    small = (
        scale_query[0],
        scale_key[0],
        scale_value[0],
        norms.transpose(1, 0, 2, 3).reshape(-1).astype(jnp.bfloat16),
    )
    got_early, far_early, done = lax.optimization_barrier((got_early, far_early, done))
    sides = send(far_early, (False, 1, 0)), send(got_early, (False, 0, 1))
    new_query = blended(
        ranks, first, new_query, query, (got_early, far_early), sides, done
    )
    got_query, new_query = lax.optimization_barrier((got_query, new_query))
    new_query = blended(
        ranks, first + span, new_query, query, [got_query] * 2, [to_side(got_query)] * 2, done
    )
    got_key, new_query = lax.optimization_barrier((got_key, new_query))
    new_key = blended(ranks, 0, done, key, [got_key] * 2, [to_side(got_key)] * 2, done)
    got_value, new_key, small = lax.optimization_barrier((got_value, new_key, small))
    side_value = to_side(got_value)
    side_rest = to_side(got_rest)
    new_value = placed(ranks, 0, new_value, got_value, side_value)
    new_value = placed(ranks, depth - tail, new_value, got_rest, side_rest)
    return (new_query, new_key, new_value, *small)


def solution(mesh):
    in_specs = (
        P(("site", "rows"), "width"),
        P(("site", "rows"), "width"),
        P(("site", "rows"), "width"),
        P(("site", "rows"), "width"),
        P(("site", "rows"), "width"),
        P(("site", "rows"), "width"),
        P(("site", "rows")),
        P(("site", "rows", "width")),
        P(("site", "rows", "width")),
    )
    out_specs = (
        P("site", "width"),
        P("site", "width"),
        P("site", "width"),
        P(("site", "width")),
        P(("site", "width")),
        P(("site", "width")),
        P("site"),
    )
    body = functools.partial(shards, mesh.shape["rows"], mesh.shape["width"])

    return jax.shard_map(
        body, mesh=mesh, in_specs=in_specs, out_specs=out_specs, check_vma=False
    )
```
